128 devices in a mesh: rows: 8 (over y_hi, z), bundle: 16 (over y_lo, x, core).
Axes of the slice: x: 4, y: 4 (y_hi: 2, y_lo: 2; y = y_hi * 2 + y_lo), z: 4, core: 2. Of those that a mesh axis runs over, the one named last changes fastest.
Arguments:
- raw_values: float32 [32768, 4096], P(('rows', 'bundle')), may hold values from -2100 to 2100
- bin_edges: float32 [4096, 255], P(('rows', 'bundle')), may hold values from -2100 to 2100, as said below
- feature_column: int32 [4096], replicated, may hold values from 0 to 4095, each once
- bin_offset: int32 [4096], replicated, may hold values from 0 to 63
Outputs:
- bin_codes: int32 [32768, 4096], P('rows', 'bundle')
The draws below stay inside these ranges and needn't reach their ends.
Inputs may be any that keep to these rules, and one draw needn't show every extreme that they name: Every row of bin_edges is strictly increasing. `feature_column`: each column 0 .. 4095 is named once.
All inputs are finite; a program needn't handle non-finite values.
Results may differ from the reference program's by a relative error of at most 0.0003.
Values may be sent and summed in bfloat16 or wider, within the bound.
No kernel may reach another device: no remote copies, remote signals or barrier semaphores. Data moves between devices by JAX's collectives and lax.ppermute only.
A program may use at most 64 MiB of HBM per device.

```python
import math
import jax
import jax.numpy as jnp
from jax import lax

FEATURE_COUNT = 4096
BOUNDARY_COUNT = 255
ROWS = 32768


def feature_frame(key):
    center_key = jax.random.fold_in(key, 21)
    stretch_key = jax.random.fold_in(key, 22)
    magnitude = jax.random.uniform(center_key, (FEATURE_COUNT,), jnp.float32, 256.0, 2048.0)
    center = magnitude
    stretch = jnp.exp(jax.random.uniform(stretch_key, (FEATURE_COUNT,), jnp.float32, -0.69, 0.69))
    return (center, stretch)


def draw_raw_values(key, part):
    center, stretch = feature_frame(key)
    noise_key = jax.random.fold_in(key, 31)
    unit = jax.random.truncated_normal(noise_key, -6.0, 6.0, (ROWS, FEATURE_COUNT), jnp.float32)
    return (center[None, :] + stretch[None, :] * unit).astype(jnp.float32)


def draw_bin_edges(key, part):
    center, stretch = feature_frame(key)
    steps_key = jax.random.fold_in(key, 11)
    spike_random_key = jax.random.fold_in(key, 12)
    step_increments = jnp.exp(jax.random.uniform(steps_key, (FEATURE_COUNT, BOUNDARY_COUNT), jnp.float32, -3.0, 0.69))
    edge_positions = jax.random.randint(spike_random_key, (FEATURE_COUNT, 3), 0, BOUNDARY_COUNT)
    column_values = jnp.arange(BOUNDARY_COUNT, dtype=jnp.int32)
    spike_values = jnp.any(column_values[None, :, None] == edge_positions[:, None, :], axis=2)
    step_increments = step_increments * jnp.where(spike_values, 30.0, 1.0)
    running = jnp.cumsum(step_increments, axis=1)
    unit = -3.0 + 6.0 * running / (running[:, -1:] + 1.0)
    edges = center[:, None] + stretch[:, None] * unit
    return edges.astype(jnp.float32)


def place_ends(values, key, least, largest):
    index_at = [jax.random.randint(jax.random.fold_in(key, axis), (), 0, length) for axis, length in enumerate(values.shape)]
    widest = values.shape.index(max(values.shape))
    next_to = index_at[:widest] + [(index_at[widest] + 1) % values.shape[widest]] + index_at[widest + 1:]
    return values.at[tuple(index_at)].set(least).at[tuple(next_to)].set(largest)


def setup_inputs(seed: int = 0) -> dict:
    key_of = jax.random.split(jax.random.key(seed), 5)
    return {
        "raw_values": draw_raw_values(jax.random.fold_in(key_of[4], 71), 0),
        "bin_edges": draw_bin_edges(jax.random.fold_in(key_of[4], 71), 0),
        "feature_column": jax.random.permutation(key_of[2], FEATURE_COUNT).astype(jnp.int32),
        "bin_offset": place_ends(jax.random.randint(key_of[3], (FEATURE_COUNT,), 0, 64), jax.random.fold_in(key_of[3], 1), 0, 63).astype(jnp.int32),
    }


def count_below(values, edges):
    total = values.shape[0]
    block = math.gcd(total, 512)

    def one_block(part_rows):
        return jnp.sum(part_rows[:, :, None] > edges[None, :, :], axis=2, dtype=jnp.int32)

    blocks = values.reshape(total // block, block, values.shape[1])
    return lax.map(one_block, blocks).reshape(total, values.shape[1])


def reference(raw_values, bin_edges, feature_column, bin_offset):
    count_feat = feature_column.shape[0]
    owner_feature = jnp.zeros((count_feat,), jnp.int32).at[feature_column].set(jnp.arange(count_feat, dtype=jnp.int32))
    ordered = jnp.take(raw_values, owner_feature, axis=1)
    edges = jnp.take(bin_edges, owner_feature, axis=0)
    bins = count_below(ordered, edges)
    return bins + jnp.take(bin_offset, owner_feature)[None, :]
```

```python
import jax
import jax.numpy as jnp
from jax import lax
from jax.experimental import pallas as pl
from jax.experimental.pallas import tpu as pltpu
from jax.sharding import PartitionSpec as P

AXES = ("rows", "bundle")
CHUNKS = 2
WIDE = 4
SIDE = 4


def device_at(y, z, x, core):
    return ((y // 2) * 4 + z) * 16 + (y % 2) * 8 + x * 2 + core


def gather_groups():
    ring = range(SIDE)
    planes = [[device_at(y, z, x, 0) for y in ring for x in ring] for z in ring]
    planes += [[device_at(y, z, x, 1) for z in ring for y in ring] for x in ring]
    lines = [[device_at(y, z, x, 0) for z in ring] for y in ring for x in ring]
    lines += [[device_at(y, z, x, 1) for x in ring] for z in ring for y in ring]
    return planes, lines


def spread(piece, groups):
    copies = jnp.broadcast_to(piece[None], (len(groups[0]), *piece.shape))
    return lax.all_to_all(copies, AXES, split_axis=0, concat_axis=0, axis_index_groups=groups, tiled=True)


def gather_edges(bin_edges):
    planes, lines = gather_groups()
    padded = jnp.pad(bin_edges, ((0, 0), (0, 1)))
    plane = spread(padded, planes)
    mine = spread(plane, lines).reshape(64, 32, 256)
    other = lax.ppermute(mine, "bundle", [(i, i ^ 1) for i in range(16)])
    return mine, other


def pick(table, index):
    dims = lax.GatherDimensionNumbers(
        offset_dims=(),
        collapsed_slice_dims=(0,),
        start_index_map=(0,),
        operand_batching_dims=(1,),
        start_indices_batching_dims=(1,),
    )
    return lax.gather(
        table, index[..., None], dims, (1, 1), mode=lax.GatherScatterMode.PROMISE_IN_BOUNDS
    )


def count_steps(values, table):
    top = table(31)
    group = jnp.where(values > jnp.broadcast_to(top[3:4], values.shape), 4, 0)
    group = jnp.where(values > pick(top, group + 1), group + 2, group)
    group = jnp.where(values > pick(top, group), group + 1, group)

    def at(o):
        return pick(table(o), group)

    b4 = values > at(15)
    b5 = values > jnp.where(b4, at(23), at(7))
    b6 = values > jnp.where(b4, jnp.where(b5, at(27), at(19)), jnp.where(b5, at(11), at(3)))

    def among(o):
        pairs = [jnp.where(b6, at(8 * i + 4 + o), at(8 * i + o)) for i in range(4)]
        return jnp.where(b4, jnp.where(b5, pairs[3], pairs[2]), jnp.where(b5, pairs[1], pairs[0]))

    b7 = values > among(1)
    b8 = values > jnp.where(b7, among(2), among(0))
    count = group * 32
    for bit, weight in ((b4, 16), (b5, 8), (b6, 4), (b7, 2), (b8, 1)):
        count = count + jnp.where(bit, weight, 0)
    return count


def bin_kernel(core_ref, raw_ref, mine_ref, other_ref, column_ref, offset_ref, out_ref, edges, tables, codes, sems):
    core = core_ref[0]
    height = raw_ref.shape[0]
    places = [(y, z, x, side) for y in range(SIDE) for z in range(SIDE) for x in range(SIDE) for side in range(2)]

    def piece(y, z, x, side):
        whose = core if side == 0 else 1 - core
        flat = z * 16 + y * 4 + x
        cross = x * 16 + z * 4 + y
        source = flat + whose * (cross - flat)
        where = device_at(y, z, x, 0) + whose
        ref = mine_ref if side == 0 else other_ref
        return pltpu.make_async_copy(
            ref.at[source], edges.at[pl.ds(where * 32, 32), :], sems.at[device_at(y, z, x, side)]
        )

    for place in places:
        piece(*place).start()
    for place in places:
        piece(*place).wait()

    codes[height:, :] = jnp.zeros((16, codes.shape[1]), codes.dtype)
    codes[height : height + 8, :] = jnp.broadcast_to(
        offset_ref[...].astype(jnp.float32), (8, codes.shape[1])
    ).astype(codes.dtype)

    def one_block(j, carry):
        lanes = pl.ds(pl.multiple_of(j * 128, 128), 128)
        tables[...] = edges[lanes, :].T

        def table(o):
            return tables[pl.ds(o, 8, stride=32), :]

        def some_rows(i, inner):
            parts = []
            for w in range(WIDE):
                rows = pl.ds(pl.multiple_of((i * WIDE + w) * 8, 8), 8)
                parts.append(count_steps(raw_ref[rows, lanes], table))
            whole = jnp.concatenate(parts, axis=0).astype(jnp.float32)
            rows = pl.ds(pl.multiple_of(i * WIDE * 8, WIDE * 8), WIDE * 8)
            codes[rows, lanes] = whole.astype(codes.dtype)
            return inner

        return lax.fori_loop(0, height // (8 * WIDE), some_rows, carry)

    lax.fori_loop(0, codes.shape[1] // 128, one_block, 0)

    span = out_ref.shape[2]

    def one_bundle(d, carry):
        column = column_ref[...] - d * span
        lines = lax.broadcasted_iota(jnp.int32, (span, column.shape[1]), 0)
        chosen = jnp.where(lines == column, 1.0, 0.0).astype(jnp.bfloat16)
        moved = lax.dot_general(
            codes[...], chosen, (((1,), (1,)), ((), ())), preferred_element_type=jnp.float32
        )
        total = moved[:height] + moved[height : height + 1]
        out_ref[d] = total.astype(jnp.int32).astype(jnp.int16)
        return carry

    lax.fori_loop(0, out_ref.shape[0], one_bundle, 0)


def bin_rows(core, raw, part, mine, other, column, offset):
    height = raw.shape[0] // CHUNKS
    count_feat = raw.shape[1]
    span = 256
    return pl.pallas_call(
        bin_kernel,
        grid_spec=pltpu.PrefetchScalarGridSpec(
            num_scalar_prefetch=1,
            grid=(1,),
            in_specs=[
                pl.BlockSpec((height, count_feat), lambda i, c: (part, 0)),
                pl.BlockSpec(memory_space=pltpu.HBM),
                pl.BlockSpec(memory_space=pltpu.HBM),
                pl.BlockSpec((1, count_feat), lambda i, c: (0, 0)),
                pl.BlockSpec((1, count_feat), lambda i, c: (0, 0)),
            ],
            out_specs=pl.BlockSpec((count_feat // span, height, span), lambda i, c: (0, 0, 0)),
            scratch_shapes=[
                pltpu.VMEM((count_feat, 256), jnp.float32),
                pltpu.VMEM((256, 128), jnp.float32),
                pltpu.VMEM((height + 16, count_feat), jnp.bfloat16),
                pltpu.SemaphoreType.DMA((128,)),
            ],
        ),
        out_shape=jax.ShapeDtypeStruct((count_feat // span, height, span), jnp.int16),
        name=f"bin_rows_{part}",
    )(core, raw, mine, other, column, offset)


def local(raw_values, bin_edges, feature_column, bin_offset):
    core = (lax.axis_index("bundle") % 2).astype(jnp.int32).reshape(1)
    mine, other = gather_edges(bin_edges)
    arrived = []
    for part in range(CHUNKS):
        sent = bin_rows(core, raw_values, part, mine, other, feature_column[None], bin_offset[None])
        arrived.append(lax.all_to_all(sent, "bundle", split_axis=0, concat_axis=0, tiled=True))
    codes = jnp.stack(arrived, axis=1)
    return codes.reshape(-1, codes.shape[-1]).astype(jnp.int32)


def solution(mesh):
    in_specs = (P(AXES, None), P(AXES, None), P(), P())
    return jax.shard_map(local, mesh=mesh, in_specs=in_specs, out_specs=P("rows", "bundle"), check_vma=False)
```

```python
import jax
import jax.numpy as jnp
from jax import lax
from jax.experimental import pallas as pl
from jax.experimental.pallas import tpu as pltpu
from jax.sharding import PartitionSpec as P

AXES = ("rows", "bundle")
WIDE = 4
SIDE = 4
PIECE = 32
EDGES = 256
SPAN = 256


def device_at(y, z, x, core):
    return ((y // 2) * 4 + z) * 16 + (y % 2) * 8 + x * 2 + core


def from_neighbour(value, axis, step):
    pairs = []
    for y in range(SIDE):
        for z in range(SIDE):
            for x in range(SIDE):
                for core in range(2):
                    at = {"y": y, "z": z, "x": x}
                    at[axis] = (at[axis] + step) % SIDE
                    pairs.append((device_at(at["y"], at["z"], at["x"], core), device_at(y, z, x, core)))
    return lax.ppermute(value, AXES, pairs)


def swap_cores(value):
    return lax.ppermute(value, "bundle", [(i, i ^ 1) for i in range(16)])


def to_chip(value, dy, dx):
    pairs = []
    for y in range(2):
        for x in range(SIDE):
            for core in range(2):
                pairs.append((y * 8 + x * 2 + core, (y ^ dy) * 8 + ((x + dx) % SIDE) * 2 + core))
    return lax.ppermute(value, "bundle", pairs)


def ring(piece, axis):
    return jnp.stack([piece] + [from_neighbour(piece, axis, step) for step in (1, 2, 3)])


def gather_edges(bin_edges):
    padded = jnp.pad(bin_edges, ((0, 0), (0, 1)))
    ordered = padded.reshape(PIECE, 8, 32).transpose(0, 2, 1).reshape(PIECE, EDGES)
    plane = ring(ring(ordered, "y"), "x").reshape(16, PIECE, EDGES)
    up = from_neighbour(plane, "z", 1)
    down = from_neighbour(plane, "z", -1)
    far = jnp.concatenate([from_neighbour(up[:8], "z", 1), from_neighbour(down[8:], "z", -1)])
    return {0: plane, 1: up, 3: down, 2: far}


def pick(table, index):
    dims = lax.GatherDimensionNumbers(
        offset_dims=(),
        collapsed_slice_dims=(0,),
        start_index_map=(0,),
        operand_batching_dims=(1,),
        start_indices_batching_dims=(1,),
    )
    return lax.gather(
        table, index[..., None], dims, (1, 1), mode=lax.GatherScatterMode.PROMISE_IN_BOUNDS
    )


def count_below(values, table):
    top = table(31)
    group = jnp.where(values > jnp.broadcast_to(top[3:4], values.shape), 4, 0)
    group = jnp.where(values > pick(top, group + 1), group + 2, group)
    group = jnp.where(values > pick(top, group), group + 1, group)

    def at(o):
        return pick(table(o), group)

    b4 = values > at(15)
    b5 = values > jnp.where(b4, at(23), at(7))
    b6 = values > jnp.where(b4, jnp.where(b5, at(27), at(19)), jnp.where(b5, at(11), at(3)))

    def among(o):
        pairs = [jnp.where(b6, at(8 * i + 4 + o), at(8 * i + o)) for i in range(4)]
        return jnp.where(b4, jnp.where(b5, pairs[3], pairs[2]), jnp.where(b5, pairs[1], pairs[0]))

    b7 = values > among(1)
    b8 = values > jnp.where(b7, among(2), among(0))
    count = group * 32
    for bit, weight in ((b4, 16), (b5, 8), (b6, 4), (b7, 2), (b8, 1)):
        count = count + jnp.where(bit, weight, 0)
    return count


def bin_kernel(place_ref, raw_ref, mine_ref, other_ref, out_ref, edges, tables):
    my_y, my_x, core = place_ref[0], place_ref[1], place_ref[2]
    height = raw_ref.shape[0]
    half = pl.program_id(0)
    for low in range(2):
        y_step = (half * 2 + low - my_y) % SIDE
        for m in range(2):
            for s in range(2):
                index = ((2 * m + s - my_x) % SIDE) * 4 + y_step
                edges[pl.ds(pl.multiple_of((2 * s + core) * PIECE, PIECE), PIECE), :] = mine_ref[index]
                edges[pl.ds(pl.multiple_of((2 * s + 1 - core) * PIECE, PIECE), PIECE), :] = other_ref[index]
            tables[...] = edges[...].T
            lanes = slice((low * 2 + m) * 128, (low * 2 + m + 1) * 128)

            def some_rows(i, inner):
                parts = []
                for w in range(WIDE):
                    rows = pl.ds(pl.multiple_of((i * WIDE + w) * 8, 8), 8)
                    parts.append(
                        count_below(raw_ref[rows, lanes], lambda o: tables[8 * o : 8 * o + 8, :])
                    )
                whole = jnp.concatenate(parts, axis=0).astype(jnp.float32)
                rows = pl.ds(pl.multiple_of(i * WIDE * 8, WIDE * 8), WIDE * 8)
                out_ref[rows, lanes] = whole.astype(out_ref.dtype)
                return inner

            lax.fori_loop(0, height // (8 * WIDE), some_rows, 0)


def bin_slice(place, slot, raw, mine, other):
    height = raw.shape[0]
    whole = pl.BlockSpec((16, PIECE, EDGES), lambda i, p: (0, 0, 0))
    return pl.pallas_call(
        bin_kernel,
        grid_spec=pltpu.PrefetchScalarGridSpec(
            num_scalar_prefetch=1,
            grid=(2,),
            in_specs=[
                pl.BlockSpec((height, 512), lambda i, p: (0, i * 4 + p[3 + slot])),
                whole,
                whole,
            ],
            out_specs=pl.BlockSpec((height, 512), lambda i, p: (0, i)),
            scratch_shapes=[pltpu.VMEM((128, EDGES), jnp.float32), pltpu.VMEM((EDGES, 128), jnp.float32)],
        ),
        out_shape=jax.ShapeDtypeStruct((height, 1024), jnp.bfloat16),
        name=f"bin_slice_{slot}",
    )(place, raw, mine, other)


def move_kernel(place_ref, *refs, targets):
    own, sibling = refs[:4], refs[4:8]
    column_ref, offset_ref = refs[8:10]
    outs = refs[10 : 10 + len(targets)]
    codes = refs[-1]
    core = place_ref[2]
    height = own[0].shape[0]
    for slot in range(4):
        lanes = slice(slot * 1024, (slot + 1) * 1024)
        codes[pl.ds(pl.multiple_of(core * height, height), height), lanes] = own[slot][...]
        codes[pl.ds(pl.multiple_of((1 - core) * height, height), height), lanes] = sibling[slot][...]
    both = 2 * height
    codes[both:, :] = jnp.broadcast_to(offset_ref[...].astype(jnp.float32), (16, 4096)).astype(codes.dtype)
    for out_ref, (dy, dx) in zip(outs, targets):
        bundle = (place_ref[7] ^ dy) * 8 + ((place_ref[1] + dx) % SIDE) * 2 + core
        column = column_ref[...] - bundle * SPAN
        lines = lax.broadcasted_iota(jnp.int32, (SPAN, column.shape[1]), 0)
        chosen = jnp.where(lines == column, 1.0, 0.0).astype(jnp.bfloat16)
        moved = lax.dot_general(
            codes[...], chosen, (((1,), (1,)), ((), ())), preferred_element_type=jnp.float32
        )
        total = moved[:both] + moved[both : both + 1]
        out_ref[...] = total.astype(jnp.int32).astype(jnp.int16)


def move_codes(place, own, sibling, column, offset, targets, name):
    height = own[0].shape[0]
    part = pl.BlockSpec((height, 1024), lambda i, p: (0, 0))
    row = pl.BlockSpec((1, 4096), lambda i, p: (0, 0))
    return pl.pallas_call(
        lambda *refs: move_kernel(*refs, targets=targets),
        grid_spec=pltpu.PrefetchScalarGridSpec(
            num_scalar_prefetch=1,
            grid=(1,),
            in_specs=[part] * 8 + [row] * 2,
            out_specs=[pl.BlockSpec((2 * height, SPAN), lambda i, p: (0, 0))] * len(targets),
            scratch_shapes=[pltpu.VMEM((2 * height + 16, 4096), jnp.bfloat16)],
        ),
        out_shape=[jax.ShapeDtypeStruct((2 * height, SPAN), jnp.int16)] * len(targets),
        name=name,
    )(place, *own, *sibling, column, offset)


def widen_kernel(place_ref, *refs):
    out_ref = refs[-1]
    for k, ref in enumerate(refs[:-1]):

        @pl.when(pl.program_id(0) == k)
        def _():
            out_ref[...] = ref[...].astype(jnp.int32)


def widen(block, arrived):
    height = arrived[0].shape[0]
    return pl.pallas_call(
        widen_kernel,
        grid_spec=pltpu.PrefetchScalarGridSpec(
            num_scalar_prefetch=1,
            grid=(len(arrived),),
            in_specs=[pl.BlockSpec((height, SPAN), lambda i, p: (0, 0))] * len(arrived),
            out_specs=pl.BlockSpec((height, SPAN), lambda i, p: (p[i], 0)),
        ),
        out_shape=jax.ShapeDtypeStruct((8 * height, SPAN), jnp.int32),
        name="widen",
    )(block, *arrived)


def by_slice(vector, z):
    grid = vector.reshape(2, SIDE, 512)
    turned = lax.dynamic_slice_in_dim(jnp.concatenate([grid, grid], axis=1), z, SIDE, axis=1)
    return turned.transpose(1, 0, 2).reshape(1, -1)


def local(raw_values, bin_edges, feature_column, bin_offset):
    row, bundle = lax.axis_index("rows"), lax.axis_index("bundle")
    y_low, x, core = bundle // 8, (bundle // 2) % SIDE, bundle % 2
    z = row % SIDE
    place = jnp.stack(
        [(row // SIDE) * 2 + y_low, x, core] + [(z + d) % SIDE for d in range(SIDE)] + [y_low]
    ).astype(jnp.int32)
    column, offset = by_slice(feature_column, z), by_slice(bin_offset, z)
    slices = gather_edges(bin_edges)
    own, sibling = [None] * SIDE, [None] * SIDE
    for slot in (0, 1, 3, 2):
        own[slot] = bin_slice(place, slot, raw_values, slices[slot], swap_cores(slices[slot]))
        sibling[slot] = swap_cores(own[slot])
    batches = [[(1, 0), (1, 1), (0, 3)], [(0, 1), (1, 3), (1, 2)], [(0, 2), (0, 0)]]
    arrived, block = [], []
    for n, targets in enumerate(batches):
        moved = move_codes(place, own, sibling, column, offset, targets, f"move_codes_{n}")
        for (dy, dx), value in zip(targets, moved):
            arrived.append(to_chip(value, dy, dx) if (dy, dx) != (0, 0) else value)
            block.append((y_low ^ dy) * SIDE + (x - dx) % SIDE)
    return widen(jnp.stack(block).astype(jnp.int32), arrived)


def solution(mesh):
    in_specs = (P(AXES, None), P(AXES, None), P(), P())
    return jax.shard_map(local, mesh=mesh, in_specs=in_specs, out_specs=P("rows", "bundle"), check_vma=False)
```

```python
import jax
import jax.numpy as jnp
from jax import lax
from jax.experimental import pallas as pl
from jax.experimental.pallas import tpu as pltpu
from jax.sharding import PartitionSpec as P

AXES = ("rows", "bundle")
SIDE = 4
PIECE = 32
EDGES = 256
SPAN = 256
FEATURES = 4096
GROUP = 256


def device_at(y, z, x, core):
    return ((y // 2) * 4 + z) * 16 + (y % 2) * 8 + x * 2 + core


def planes():
    ring = range(SIDE)
    return [[device_at(y, z, x, core) for y in ring for x in ring] for z in ring for core in range(2)]


def along_z(value, step):
    pairs = [(h * SIDE + (z + step) % SIDE, h * SIDE + z) for h in range(2) for z in range(SIDE)]
    return lax.ppermute(value, "rows", pairs)


def swap_cores(value):
    return lax.ppermute(value, "bundle", [(i, i ^ 1) for i in range(16)])


def pick(table, index):
    dims = lax.GatherDimensionNumbers(
        offset_dims=(),
        collapsed_slice_dims=(0,),
        start_index_map=(0,),
        operand_batching_dims=(1,),
        start_indices_batching_dims=(1,),
    )
    return lax.gather(
        table, index[..., None], dims, (1, 1), mode=lax.GatherScatterMode.PROMISE_IN_BOUNDS
    )


def count_below(values, table):
    top = table(31)
    group = jnp.where(values > jnp.broadcast_to(top[3:4], values.shape), 4, 0)
    group = jnp.where(values > pick(top, group + 1), group + 2, group)
    group = jnp.where(values > pick(top, group), group + 1, group)

    def at(o):
        return pick(table(o), group)

    b4 = values > at(15)
    b5 = values > jnp.where(b4, at(23), at(7))
    b6 = values > jnp.where(b4, jnp.where(b5, at(27), at(19)), jnp.where(b5, at(11), at(3)))

    def among(o):
        pairs = [jnp.where(b6, at(8 * i + 4 + o), at(8 * i + o)) for i in range(4)]
        return jnp.where(b4, jnp.where(b5, pairs[3], pairs[2]), jnp.where(b5, pairs[1], pairs[0]))

    b7 = values > among(1)
    b8 = values > jnp.where(b7, among(2), among(0))
    count = group * 32
    for bit, weight in ((b4, 16), (b5, 8), (b6, 4), (b7, 2), (b8, 1)):
        count = count + jnp.where(bit, weight, 0)
    return count


def prep_kernel(column_ref, raw_ref, out_ref, turned):
    i = pl.program_id(0)
    slot = i % 2

    @pl.when(i == 0)
    def _():
        flat = raw_ref[...].T
        turned[0, :, 0, :] = flat[:, :128]
        turned[0, :, 1, :] = flat[:, 128:]

    @pl.when(i > 0)
    def _():
        flat = raw_ref[...].T
        base = (i - 1) * GROUP
        for start in range(0, GROUP, 16):
            rows = [turned[1 - slot, start + k] for k in range(16)]
            for k in range(16):
                out_ref[column_ref[base + start + k]] = rows[k]
        turned[slot, :, 0, :] = flat[:, :128]
        turned[slot, :, 1, :] = flat[:, 128:]


def prep(column, raw):
    count = FEATURES // GROUP
    return pl.pallas_call(
        prep_kernel,
        grid_spec=pltpu.PrefetchScalarGridSpec(
            num_scalar_prefetch=1,
            grid=(count + 1,),
            in_specs=[pl.BlockSpec((256, GROUP), lambda i, c: (0, jnp.minimum(i, count - 1)))],
            out_specs=pl.BlockSpec((FEATURES, 2, 128), lambda i, c: (0, 0, 0)),
            scratch_shapes=[pltpu.VMEM((2, GROUP, 2, 128), jnp.float32)],
        ),
        out_shape=jax.ShapeDtypeStruct((FEATURES, 2, 128), jnp.float32),
        name="prep",
    )(column, raw)


def choose_kernel(row_ref, mine_ref, other_ref, out_ref, pool):
    pool[0:512, :] = mine_ref[...]
    pool[512:1024, :] = other_ref[...]
    pool[1024:1032, :] = jnp.zeros((8, EDGES), jnp.float32)

    def eight(i, carry):
        rows = [pool[pl.ds(row_ref[i * 8 + k], 1), :] for k in range(8)]
        out_ref[pl.ds(pl.multiple_of(i * 8, 8), 8), :] = jnp.concatenate(rows, axis=0)
        return carry

    lax.fori_loop(0, SPAN // 8, eight, 0)


def choose(row, mine, other):
    whole = pl.BlockSpec((512, EDGES), lambda i, r: (0, 0))
    return pl.pallas_call(
        choose_kernel,
        grid_spec=pltpu.PrefetchScalarGridSpec(
            num_scalar_prefetch=1,
            grid=(1,),
            in_specs=[whole, whole],
            out_specs=pl.BlockSpec((SPAN, EDGES), lambda i, r: (0, 0)),
            scratch_shapes=[pltpu.VMEM((1032, EDGES), jnp.float32)],
        ),
        out_shape=jax.ShapeDtypeStruct((SPAN, EDGES), jnp.float32),
        name="choose",
    )(row, mine, other)


def table_kernel(a_ref, b_ref, c_ref, d_ref, out_ref):
    total = (a_ref[...] + b_ref[...]) + (c_ref[...] + d_ref[...])
    out_ref[...] = total.T


def make_table(parts):
    return pl.pallas_call(
        table_kernel, out_shape=jax.ShapeDtypeStruct((EDGES, SPAN), jnp.float32), name="make_table"
    )(*parts)


def bin_kernel(in_ref, table_ref, offset_ref, out_ref, turned):
    slot = pl.program_id(0) % 2
    for tile in range(4):
        high, side = tile // 2, tile % 2
        lanes = slice(side * 128, side * 128 + 128)
        turned[slot, tile] = in_ref[0, pl.ds(side * 256 + high, 128, stride=2), :].T
        offset = jnp.broadcast_to(offset_ref[:, lanes], (8, 128))

        def some_rows(i, carry):
            for w in range(4):
                rows = pl.ds(pl.multiple_of((i * 4 + w) * 8, 8), 8)
                count = count_below(
                    turned[1 - slot, tile, rows, :], lambda o: table_ref[8 * o : 8 * o + 8, lanes]
                )
                out_ref[pl.ds(pl.multiple_of(high * 128 + (i * 4 + w) * 8, 8), 8), lanes] = count + offset
            return carry

        lax.fori_loop(0, 4, some_rows, 0)


def bin_all(arrived, table, offset):
    return pl.pallas_call(
        bin_kernel,
        grid=(17,),
        in_specs=[
            pl.BlockSpec((1, 512, 128), lambda g: (jnp.minimum(g, 15), 0, 0)),
            pl.BlockSpec((EDGES, SPAN), lambda g: (0, 0)),
            pl.BlockSpec((1, SPAN), lambda g: (0, 0)),
        ],
        out_specs=pl.BlockSpec((256, SPAN), lambda g: (jnp.maximum(g - 1, 0), 0)),
        out_shape=jax.ShapeDtypeStruct((16 * 256, SPAN), jnp.int32),
        scratch_shapes=[pltpu.VMEM((2, 4, 128, 128), jnp.float32)],
        name="bin_all",
    )(arrived, table, offset)


def local(raw_values, bin_edges, feature_column, bin_offset):
    row, bundle = lax.axis_index("rows"), lax.axis_index("bundle")
    z, core = row % SIDE, bundle % 2
    padded = jnp.pad(bin_edges, ((0, 0), (0, 1)))
    ordered = padded.reshape(PIECE, 8, 32).transpose(0, 2, 1).reshape(PIECE, EDGES)
    copies = jnp.broadcast_to(ordered[None], (16, PIECE, EDGES))
    mine = lax.all_to_all(copies, AXES, split_axis=0, concat_axis=0, axis_index_groups=planes(), tiled=True)
    mine = mine.reshape(512, EDGES)

    sent = prep(feature_column, raw_values).reshape(16, 512, 128)
    sent, mine = lax.optimization_barrier((sent, mine))
    arrived = lax.all_to_all(sent, "bundle", split_axis=0, concat_axis=0, tiled=True)

    wanted = bundle * SPAN + jnp.arange(SPAN, dtype=jnp.int32)
    named = feature_column[None, :] == wanted[:, None]
    feature = jnp.max(jnp.where(named, jnp.arange(FEATURES, dtype=jnp.int32)[None], 0), axis=1)
    offset = jnp.max(jnp.where(named, bin_offset[None], 0), axis=1)
    device = feature // PIECE
    y = (device // 64) * 2 + (device // 8) % 2
    spot = (y * SIDE + (device // 2) % SIDE) * PIECE + feature % PIECE
    spot = jnp.where(device % 2 == core, spot, spot + 512)
    spot = jnp.where((device // 16) % SIDE == z, spot, 1024)
    part = choose(spot, mine, swap_cores(mine))
    table = make_table([part] + [along_z(part, step) for step in (1, 3, 2)])
    return bin_all(arrived, table, offset[None])


def solution(mesh):
    in_specs = (P(AXES, None), P(AXES, None), P(), P())
    return jax.shard_map(local, mesh=mesh, in_specs=in_specs, out_specs=P("rows", "bundle"), check_vma=False)
```

```python
import jax
import jax.numpy as jnp
from jax import lax
from jax.experimental import pallas as pl
from jax.experimental.pallas import tpu as pltpu
from jax.sharding import PartitionSpec as P

AXES = ("rows", "bundle")
SIDE = 4
PIECE = 32
EDGES = 256
SPAN = 256
FEATURES = 4096
GROUP = 1024
SUB = 256


def device_at(y, z, x, core):
    return ((y // 2) * 4 + z) * 16 + (y % 2) * 8 + x * 2 + core


def planes():
    ring = range(SIDE)
    return [[device_at(y, z, x, core) for y in ring for x in ring] for z in ring for core in range(2)]


def along_z(value, step):
    pairs = [(h * SIDE + (z + step) % SIDE, h * SIDE + z) for h in range(2) for z in range(SIDE)]
    return lax.ppermute(value, "rows", pairs)


def swap_cores(value):
    return lax.ppermute(value, "bundle", [(i, i ^ 1) for i in range(16)])


def to_member(value, dy, dx, dc):
    pairs = []
    for y in range(2):
        for x in range(SIDE):
            for core in range(2):
                target = (y ^ dy) * 8 + (x + dx) % SIDE * 2 + (core ^ dc)
                pairs.append((y * 8 + x * 2 + core, target))
    return lax.ppermute(value, "bundle", pairs)


def pick(table, index):
    dims = lax.GatherDimensionNumbers(
        offset_dims=(),
        collapsed_slice_dims=(0,),
        start_index_map=(0,),
        operand_batching_dims=(1,),
        start_indices_batching_dims=(1,),
    )
    return lax.gather(
        table, index[..., None], dims, (1, 1), mode=lax.GatherScatterMode.PROMISE_IN_BOUNDS
    )


def count_below(values, table):
    top = table(31)
    group = jnp.where(values > jnp.broadcast_to(top[3:4], values.shape), 4, 0)
    group = jnp.where(values > pick(top, group + 1), group + 2, group)
    group = jnp.where(values > pick(top, group), group + 1, group)

    def at(o):
        return pick(table(o), group)

    b4 = values > at(15)
    b5 = values > jnp.where(b4, at(23), at(7))
    b6 = values > jnp.where(b4, jnp.where(b5, at(27), at(19)), jnp.where(b5, at(11), at(3)))

    def among(o):
        pairs = [jnp.where(b6, at(8 * i + 4 + o), at(8 * i + o)) for i in range(4)]
        return jnp.where(b4, jnp.where(b5, pairs[3], pairs[2]), jnp.where(b5, pairs[1], pairs[0]))

    b7 = values > among(1)
    b8 = values > jnp.where(b7, among(2), among(0))
    count = group * 32
    for bit, weight in ((b4, 16), (b5, 8), (b6, 4), (b7, 2), (b8, 1)):
        count = count + jnp.where(bit, weight, 0)
    return count


def prep_kernel(spot_ref, raw_ref, first_ref, *refs):
    others, buffer, sems, turned = refs[:16], refs[16], refs[17], refs[18:]
    i = pl.program_id(0)

    def turn(j):
        flat = raw_ref[:, j * SUB : (j + 1) * SUB].T
        turned[j][pl.ds(0, SUB, stride=2), :] = flat[:, :128]
        turned[j][pl.ds(1, SUB, stride=2), :] = flat[:, 128:]

    def scatter(j):
        base = i * GROUP + j * SUB
        for start in range(0, SUB, 32):
            rows = []
            for q in range(8):
                four = turned[j][2 * start + 8 * q : 2 * start + 8 * q + 8, :]
                rows += [four[2 * k : 2 * k + 2, :] for k in range(4)]
            for k in range(32):
                buffer[spot_ref[base + start + k]] = rows[k]

    turn(0)
    for j in range(len(turned)):
        if j + 1 < len(turned):
            turn(j + 1)
        scatter(j)

    @pl.when(i == pl.num_programs(0) - 1)
    def _():
        copies = [pltpu.make_async_copy(buffer.at[pl.ds(0, 2048)], first_ref, sems.at[16])]
        for k, ref in enumerate(others):
            copies.append(pltpu.make_async_copy(buffer.at[pl.ds(2048 + 128 * k, 128)], ref, sems.at[k]))
        for copy in copies:
            copy.start()
        for copy in copies:
            copy.wait()


def prep(spot, raw):
    return pl.pallas_call(
        prep_kernel,
        grid_spec=pltpu.PrefetchScalarGridSpec(
            num_scalar_prefetch=1,
            grid=(FEATURES // GROUP,),
            in_specs=[pl.BlockSpec((256, GROUP), lambda i, c: (0, i))],
            out_specs=[pl.BlockSpec(memory_space=pltpu.HBM)] * 17,
            scratch_shapes=[pltpu.VMEM((FEATURES, 2, 128), jnp.float32), pltpu.SemaphoreType.DMA((17,))]
            + [pltpu.VMEM((SUB * 2, 128), jnp.float32)] * (GROUP // SUB),
        ),
        out_shape=[jax.ShapeDtypeStruct((2048, 2, 128), jnp.float32)]
        + [jax.ShapeDtypeStruct((128, 2, 128), jnp.float32)] * 16,
        name="prep",
    )(spot, raw)


def choose_kernel(row_ref, mine_ref, other_ref, out_ref, pool):
    pool[0:512, :] = mine_ref[...]
    pool[512:1024, :] = other_ref[...]
    pool[1024:1032, :] = jnp.zeros((8, EDGES), jnp.float32)

    def eight(i, carry):
        rows = [pool[pl.ds(row_ref[i * 8 + k], 1), :] for k in range(8)]
        out_ref[pl.ds(pl.multiple_of(i * 8, 8), 8), :] = jnp.concatenate(rows, axis=0)
        return carry

    lax.fori_loop(0, SPAN // 8, eight, 0)


def choose(row, mine, other):
    whole = pl.BlockSpec((512, EDGES), lambda i, r: (0, 0))
    return pl.pallas_call(
        choose_kernel,
        grid_spec=pltpu.PrefetchScalarGridSpec(
            num_scalar_prefetch=1,
            grid=(1,),
            in_specs=[whole, whole],
            out_specs=pl.BlockSpec((SPAN, EDGES), lambda i, r: (0, 0)),
            scratch_shapes=[pltpu.VMEM((1032, EDGES), jnp.float32)],
        ),
        out_shape=jax.ShapeDtypeStruct((SPAN, EDGES), jnp.float32),
        name="choose",
    )(row, mine, other)


def table_kernel(a_ref, b_ref, c_ref, d_ref, out_ref):
    total = (a_ref[...] + b_ref[...]) + (c_ref[...] + d_ref[...])
    out_ref[...] = total.T


def make_table(parts):
    return pl.pallas_call(
        table_kernel, out_shape=jax.ShapeDtypeStruct((EDGES, SPAN), jnp.float32), name="make_table"
    )(*parts)


def bin_tile(values, table_ref, offset, out_ref, top, lanes):
    for r in range(0, 128, 8):
        count = count_below(values(r), lambda o: table_ref[8 * o : 8 * o + 8, lanes])
        out_ref[pl.ds(pl.multiple_of(top + r, 8), 8), :] = count + offset


def first_kernel(in_ref, table_ref, offset_ref, out_ref, turned):
    slot = pl.program_id(0) % 2
    lanes = slice(0, 128)
    offset = jnp.broadcast_to(offset_ref[:, lanes], (8, 128))

    def one_tile(high, carry):
        bin_tile(
            lambda r: turned[1 - slot, high, r : r + 8, :], table_ref, offset, out_ref, high * 128, lanes
        )
        turned[slot, high] = in_ref[0, pl.ds(high, 128, stride=2), :].T
        return carry

    lax.fori_loop(0, 2, one_tile, 0)


def bin_first(arrived, table, offset):
    return pl.pallas_call(
        first_kernel,
        grid=(17,),
        in_specs=[
            pl.BlockSpec((1, 256, 128), lambda g: (jnp.minimum(g, 15), 0, 0)),
            pl.BlockSpec((EDGES, SPAN), lambda g: (0, 0)),
            pl.BlockSpec((1, SPAN), lambda g: (0, 0)),
        ],
        out_specs=pl.BlockSpec((256, 128), lambda g: (jnp.maximum(g - 1, 0), 0)),
        out_shape=jax.ShapeDtypeStruct((16 * 256, SPAN), jnp.int32),
        scratch_shapes=[pltpu.VMEM((2, 2, 128, 128), jnp.float32)],
        name="bin_first",
    )(arrived, table, offset)


def second_kernel(source_ref, table_ref, offset_ref, *refs):
    parts, out_ref = refs[:16], refs[17]
    stage, turned, sems = refs[18:]
    g = pl.program_id(0)
    slot = g % 2
    lanes = slice(128, 256)
    offset = jnp.broadcast_to(offset_ref[:, lanes], (8, 128))

    @pl.when(g == 0)
    def _():
        for k, ref in enumerate(parts):
            pltpu.make_async_copy(ref, stage.at[k], sems.at[k]).start()

    here = jnp.minimum(g, 15)

    @pl.when(g < 16)
    def _():
        pltpu.make_async_copy(parts[0], stage.at[here], sems.at[here]).wait()

    def one_tile(high, carry):
        bin_tile(
            lambda r: turned[1 - slot, high, r : r + 8, :], table_ref, offset, out_ref, high * 128, lanes
        )
        turned[slot, high] = stage[here, pl.ds(high, 128, stride=2), :].T
        return carry

    lax.fori_loop(0, 2, one_tile, 0)


def bin_second(source, table, offset, parts, out):
    anywhere = pl.BlockSpec(memory_space=pltpu.HBM)
    return pl.pallas_call(
        second_kernel,
        grid_spec=pltpu.PrefetchScalarGridSpec(
            num_scalar_prefetch=1,
            grid=(17,),
            in_specs=[
                pl.BlockSpec((EDGES, SPAN), lambda g, s: (0, 0)),
                pl.BlockSpec((1, SPAN), lambda g, s: (0, 0)),
            ]
            + [anywhere] * 17,
            out_specs=pl.BlockSpec((256, 128), lambda g, s: (s[jnp.maximum(g - 1, 0)], 1)),
            scratch_shapes=[
                pltpu.VMEM((16, 256, 128), jnp.float32),
                pltpu.VMEM((2, 2, 128, 128), jnp.float32),
                pltpu.SemaphoreType.DMA((16,)),
            ],
        ),
        out_shape=jax.ShapeDtypeStruct(out.shape, out.dtype),
        input_output_aliases={19: 0},
        name="bin_second",
    )(source, table, offset, *parts, out)


def local(raw_values, bin_edges, feature_column, bin_offset):
    row, bundle = lax.axis_index("rows"), lax.axis_index("bundle")
    z, core = row % SIDE, bundle % 2
    padded = jnp.pad(bin_edges, ((0, 0), (0, 1)))
    ordered = padded.reshape(PIECE, 8, 32).transpose(0, 2, 1).reshape(PIECE, EDGES)
    copies = jnp.broadcast_to(ordered[None], (16, PIECE, EDGES))
    mine = lax.all_to_all(copies, AXES, split_axis=0, concat_axis=0, axis_index_groups=planes(), tiled=True)
    mine = mine.reshape(512, EDGES)

    x, y_low = (bundle // 2) % SIDE, bundle // 8
    owner, inside = feature_column // SPAN, feature_column % SPAN
    apart = (owner // 8 ^ y_low) * 8 + ((owner // 2) % SIDE - x) % SIDE * 2 + (owner % 2 ^ core)
    spot = jnp.where(inside < 128, owner * 128 + inside, 2048 + apart * 128 + inside - 128)
    first, *others = prep(spot, raw_values)
    first, mine, *others = lax.optimization_barrier((first.reshape(16, 256, 128), mine, *others))
    arrived = lax.all_to_all(first, "bundle", split_axis=0, concat_axis=0, tiled=True)
    parts, source = [], []
    for k, value in enumerate(others):
        dy, dx, dc = k // 8, (k // 2) % SIDE, k % 2
        value = value.reshape(256, 128)
        parts.append(to_member(value, dy, dx, dc) if k else value)
        source.append((y_low ^ dy) * 8 + (x - dx) % SIDE * 2 + (core ^ dc))

    wanted = bundle * SPAN + jnp.arange(SPAN, dtype=jnp.int32)
    named = feature_column[None, :] == wanted[:, None]
    feature = jnp.max(jnp.where(named, jnp.arange(FEATURES, dtype=jnp.int32)[None], 0), axis=1)
    offset = jnp.max(jnp.where(named, bin_offset[None], 0), axis=1)
    device = feature // PIECE
    far_y = (device // 64) * 2 + (device // 8) % 2
    line = (far_y * SIDE + (device // 2) % SIDE) * PIECE + feature % PIECE
    line = jnp.where(device % 2 == core, line, line + 512)
    line = jnp.where((device // 16) % SIDE == z, line, 1024)
    part = choose(line, mine, swap_cores(mine))
    table = make_table([part] + [along_z(part, step) for step in (1, 3, 2)])
    out = bin_first(arrived, table, offset[None])
    return bin_second(jnp.stack(source).astype(jnp.int32), table, offset[None], parts, out)


def solution(mesh):
    in_specs = (P(AXES, None), P(AXES, None), P(), P())
    return jax.shard_map(local, mesh=mesh, in_specs=in_specs, out_specs=P("rows", "bundle"), check_vma=False)
```

```python
import jax
import jax.numpy as jnp
from jax import lax
from jax.experimental import pallas as pl
from jax.experimental.pallas import tpu as pltpu
from jax.sharding import PartitionSpec as P


AXES = ("rows", "bundle")
SIDE = 4
PIECE = 32
EDGES = 256
SPAN = 256
FEATURES = 4096
CHIPS = 8
ORDER = ((0, 0), (1, 0), (0, 1), (0, 3), (1, 1), (1, 3), (1, 2), (0, 2))
BATCHES = (3, 2, 2, 1)
GROUP = 1024
SUB = 256


def device_at(y, z, x, core):
    return ((y // 2) * 4 + z) * 16 + (y % 2) * 8 + x * 2 + core


def planes():
    ring = range(SIDE)
    return [[device_at(y, z, x, core) for y in ring for x in ring] for z in ring for core in range(2)]


def along_z(value, step):
    pairs = [(h * SIDE + (z + step) % SIDE, h * SIDE + z) for h in range(2) for z in range(SIDE)]
    return lax.ppermute(value, "rows", pairs)


def swap_cores(value):
    return lax.ppermute(value, "bundle", [(i, i ^ 1) for i in range(16)])


def to_chip(value, dy, dx):
    pairs = []
    for y in range(2):
        for x in range(SIDE):
            for core in range(2):
                pairs.append((y * 8 + x * 2 + core, (y ^ dy) * 8 + (x + dx) % SIDE * 2 + core))
    return lax.ppermute(value, "bundle", pairs)


def pick(table, index):
    dims = lax.GatherDimensionNumbers(
        offset_dims=(),
        collapsed_slice_dims=(0,),
        start_index_map=(0,),
        operand_batching_dims=(1,),
        start_indices_batching_dims=(1,),
    )
    return lax.gather(
        table, index[..., None], dims, (1, 1), mode=lax.GatherScatterMode.PROMISE_IN_BOUNDS
    )


def count_below(values, table):
    top = table(31)
    group = jnp.where(values > jnp.broadcast_to(top[3:4], values.shape), 4, 0)
    group = jnp.where(values > pick(top, group + 1), group + 2, group)
    group = jnp.where(values > pick(top, group), group + 1, group)

    def at(o):
        return pick(table(o), group)

    b4 = values > at(15)
    b5 = values > jnp.where(b4, at(23), at(7))
    b6 = values > jnp.where(b4, jnp.where(b5, at(27), at(19)), jnp.where(b5, at(11), at(3)))

    def among(o):
        pairs = [jnp.where(b6, at(8 * i + 4 + o), at(8 * i + o)) for i in range(4)]
        return jnp.where(b4, jnp.where(b5, pairs[3], pairs[2]), jnp.where(b5, pairs[1], pairs[0]))

    b7 = values > among(1)
    b8 = values > jnp.where(b7, among(2), among(0))
    count = group * 32
    for bit, weight in ((b4, 16), (b5, 8), (b6, 4), (b7, 2), (b8, 1)):
        count = count + jnp.where(bit, weight, 0)
    return count


def prep_kernel(spot_ref, raw_ref, *refs):
    outs, buffer, sems, turned = refs[:CHIPS], refs[CHIPS], refs[CHIPS + 1], refs[CHIPS + 2 :]
    i = pl.program_id(0)

    def turn(j):
        flat = raw_ref[:, j * SUB : (j + 1) * SUB].T
        turned[j][pl.ds(0, SUB, stride=2), :] = flat[:, :128]
        turned[j][pl.ds(1, SUB, stride=2), :] = flat[:, 128:]

    def scatter(j):
        base = i * GROUP + j * SUB
        for start in range(0, SUB, 32):
            rows = []
            for q in range(8):
                four = turned[j][2 * start + 8 * q : 2 * start + 8 * q + 8, :]
                rows += [four[2 * k : 2 * k + 2, :] for k in range(4)]
            for k in range(32):
                buffer[spot_ref[base + start + k]] = rows[k]

    turn(0)
    for j in range(len(turned)):
        if j + 1 < len(turned):
            turn(j + 1)
        scatter(j)

    @pl.when(i == pl.num_programs(0) - 1)
    def _():
        copies = []
        for k, ref in enumerate(outs):
            copies.append(pltpu.make_async_copy(buffer.at[pl.ds(512 * k, 512)], ref, sems.at[k]))
        for copy in copies:
            copy.start()
        for copy in copies:
            copy.wait()


def prep(spot, raw):
    return pl.pallas_call(
        prep_kernel,
        grid_spec=pltpu.PrefetchScalarGridSpec(
            num_scalar_prefetch=1,
            grid=(FEATURES // GROUP,),
            in_specs=[pl.BlockSpec((256, GROUP), lambda i, c: (0, i))],
            out_specs=[pl.BlockSpec(memory_space=pltpu.HBM)] * CHIPS,
            scratch_shapes=[pltpu.VMEM((FEATURES, 2, 128), jnp.float32), pltpu.SemaphoreType.DMA((CHIPS,))]
            + [pltpu.VMEM((SUB * 2, 128), jnp.float32)] * (GROUP // SUB),
        ),
        out_shape=[jax.ShapeDtypeStruct((512, 2, 128), jnp.float32)] * CHIPS,
        name="prep",
    )(spot, raw)


def choose_kernel(row_ref, mine_ref, other_ref, out_ref, pool):
    pool[0:512, :] = mine_ref[...]
    pool[512:1024, :] = other_ref[...]
    pool[1024:1032, :] = jnp.zeros((8, EDGES), jnp.float32)

    def eight(i, carry):
        rows = [pool[pl.ds(row_ref[i * 8 + k], 1), :] for k in range(8)]
        out_ref[pl.ds(pl.multiple_of(i * 8, 8), 8), :] = jnp.concatenate(rows, axis=0)
        return carry

    lax.fori_loop(0, SPAN // 8, eight, 0)


def choose(row, mine, other):
    whole = pl.BlockSpec((512, EDGES), lambda i, r: (0, 0))
    return pl.pallas_call(
        choose_kernel,
        grid_spec=pltpu.PrefetchScalarGridSpec(
            num_scalar_prefetch=1,
            grid=(1,),
            in_specs=[whole, whole],
            out_specs=pl.BlockSpec((SPAN, EDGES), lambda i, r: (0, 0)),
            scratch_shapes=[pltpu.VMEM((1032, EDGES), jnp.float32)],
        ),
        out_shape=jax.ShapeDtypeStruct((SPAN, EDGES), jnp.float32),
        name="choose",
    )(row, mine, other)


def table_kernel(a_ref, b_ref, c_ref, d_ref, out_ref):
    total = (a_ref[...] + b_ref[...]) + (c_ref[...] + d_ref[...])
    out_ref[...] = total.T


def make_table(parts):
    return pl.pallas_call(
        table_kernel, out_shape=jax.ShapeDtypeStruct((EDGES, SPAN), jnp.float32), name="make_table"
    )(*parts)


def bin_kernel(row_ref, table_ref, offset_ref, *refs, count, fresh):
    own, swapped = refs[:count], refs[count : 2 * count]
    out_ref, stage, turned, result, in_sems, out_sems = refs[2 * count + (0 if fresh else 1) :]

    def take(i, side):
        source = own[i].at[0] if side == 0 else swapped[i].at[1]
        return pltpu.make_async_copy(source, stage.at[2 * i + side], in_sems.at[2 * i + side])

    def give(part):
        rows = pl.ds(pl.multiple_of(row_ref[part], 256), 256)
        return pltpu.make_async_copy(result.at[part], out_ref.at[rows, :], out_sems.at[part])

    for i in range(count):
        take(i, 0).start()
        take(i, 1).start()

    def arrive(part):
        pltpu.make_async_copy(own[0].at[0], stage.at[part], in_sems.at[part]).wait()

    def turn(tile, slot):
        line = (tile % 4 // 2) * 256 + tile % 2
        turned[slot] = stage[tile // 4, pl.ds(line, 128, stride=2), :].T

    arrive(0)
    turn(0, 0)
    last = 8 * count - 1

    def one_tile(t, carry):
        following = jnp.minimum(t + 1, last)

        @pl.when((t % 4 == 3) & (t < last))
        def _():
            arrive(following // 4)

        lanes = pl.ds(pl.multiple_of((t % 4 // 2) * 128, 128), 128)
        offset = jnp.broadcast_to(offset_ref[:, lanes], (8, 128))
        for r in range(0, 128, 8):
            below = count_below(
                turned[t % 2, r : r + 8, :], lambda o: table_ref[8 * o : 8 * o + 8, lanes]
            )
            rows = pl.ds(pl.multiple_of((t % 2) * 128 + r, 8), 8)
            result[t // 4, rows, lanes] = below + offset
        turn(following, 1 - t % 2)

        @pl.when(t % 4 == 3)
        def _():
            give(t // 4).start()

        return carry

    lax.fori_loop(0, 8 * count, one_tile, 0)
    for part in range(2 * count):
        give(part).wait()


def bin_chips(row, table, offset, own, swapped, out):
    count, fresh = len(own), out is None
    anywhere = pl.BlockSpec(memory_space=pltpu.HBM)
    return pl.pallas_call(
        lambda *refs: bin_kernel(*refs, count=count, fresh=fresh),
        grid_spec=pltpu.PrefetchScalarGridSpec(
            num_scalar_prefetch=1,
            grid=(1,),
            in_specs=[
                pl.BlockSpec((EDGES, SPAN), lambda g, s: (0, 0)),
                pl.BlockSpec((1, SPAN), lambda g, s: (0, 0)),
            ]
            + [anywhere] * (2 * count + (0 if fresh else 1)),
            out_specs=anywhere,
            scratch_shapes=[
                pltpu.VMEM((2 * count, 512, 128), jnp.float32),
                pltpu.VMEM((2, 128, 128), jnp.float32),
                pltpu.VMEM((2 * count, 256, SPAN), jnp.int32),
                pltpu.SemaphoreType.DMA((2 * count,)),
                pltpu.SemaphoreType.DMA((2 * count,)),
            ],
        ),
        out_shape=jax.ShapeDtypeStruct((16 * 256, SPAN), jnp.int32),
        input_output_aliases={} if fresh else {3 + 2 * count: 0},
    )(row, table, offset, *own, *swapped, *([] if fresh else [out]))


def step(raw_values, bin_edges, feature_column, bin_offset):
    row, bundle = lax.axis_index("rows"), lax.axis_index("bundle")
    z, core = row % SIDE, bundle % 2
    padded = jnp.pad(bin_edges, ((0, 0), (0, 1)))
    ordered = padded.reshape(PIECE, 8, 32).transpose(0, 2, 1).reshape(PIECE, EDGES)
    copies = jnp.broadcast_to(ordered[None], (16, PIECE, EDGES))
    mine = lax.all_to_all(copies, AXES, split_axis=0, concat_axis=0, axis_index_groups=planes(), tiled=True)
    mine = mine.reshape(512, EDGES)

    x, y_low = (bundle // 2) % SIDE, bundle // 8
    owner, inside = feature_column // SPAN, feature_column % SPAN
    chip = (owner // 8 ^ y_low) * SIDE + ((owner // 2) % SIDE - x) % SIDE
    spot = chip * 512 + (owner % 2 ^ core) * 256 + inside
    sent = [value.reshape(2, 512, 128) for value in prep(spot, raw_values)]
    arrived = []
    for dy, dx in ORDER:
        value = sent[dy * SIDE + dx]
        arrived.append(to_chip(value, dy, dx) if dy + dx else value)

    wanted = bundle * SPAN + jnp.arange(SPAN, dtype=jnp.int32)
    named = feature_column[None, :] == wanted[:, None]
    feature = jnp.max(jnp.where(named, jnp.arange(FEATURES, dtype=jnp.int32)[None], 0), axis=1)
    offset = jnp.max(jnp.where(named, bin_offset[None], 0), axis=1)
    device = feature // PIECE
    far_y = (device // 64) * 2 + (device // 8) % 2
    line = (far_y * SIDE + (device // 2) % SIDE) * PIECE + feature % PIECE
    line = jnp.where(device % 2 == core, line, line + 512)
    line = jnp.where((device // 16) % SIDE == z, line, 1024)
    part = choose(line, mine, swap_cores(mine))
    groups, done = [], 0
    for count in BATCHES:
        groups.append((ORDER[done : done + count], arrived[done : done + count]))
        done += count
    near, *turned = [along_z(part, step) for step in (1, 3, 2)]
    *own, near = lax.optimization_barrier((*groups[0][1], near))
    swapped = [swap_cores(value) for value in own]
    table = make_table([part, near] + turned)
    *following, table = lax.optimization_barrier((*groups[1][1], table))
    out = None
    for n, (chips, later) in enumerate(groups):
        if n == 1:
            own, swapped = following, [swap_cores(value) for value in following]
        elif n > 1:
            *own, out = lax.optimization_barrier((*later, out))
            swapped = [swap_cores(value) for value in own]
        row = []
        for dy, dx in chips:
            base = ((y_low ^ dy) * SIDE + (x - dx) % SIDE) * 512
            row += [base + core * 256, base + (1 - core) * 256]
        row = jnp.stack(row).astype(jnp.int32)
        out = bin_chips(row, table, offset[None], own, swapped, out)
    return out


def solution(mesh):
    in_specs = (P(AXES, None), P(AXES, None), P(), P())
    return jax.shard_map(step, mesh=mesh, in_specs=in_specs, out_specs=P("rows", "bundle"), check_vma=False)
```

```python
import jax
import jax.numpy as jnp
from jax import lax
from jax.experimental import pallas as pl
from jax.experimental.pallas import tpu as pltpu
from jax.sharding import PartitionSpec as P


AXES = ("rows", "bundle")
SIDE = 4
PIECE = 32
EDGES = 256
SPAN = 256
FEATURES = 4096
CHIPS = 8
PHASES = (((1, 0), (0, 2)), ((1, 1), (0, 3)), ((1, 3), (0, 1)), ((1, 2),))
GROUP = 1024
SUB = 256


def device_at(y, z, x, core):
    return ((y // 2) * 4 + z) * 16 + (y % 2) * 8 + x * 2 + core


def planes():
    ring = range(SIDE)
    return [[device_at(y, z, x, core) for y in ring for x in ring] for z in ring for core in range(2)]


def along_z(value, step):
    pairs = [(h * SIDE + (z + step) % SIDE, h * SIDE + z) for h in range(2) for z in range(SIDE)]
    return lax.ppermute(value, "rows", pairs)


def swap_cores(value):
    return lax.ppermute(value, "bundle", [(i, i ^ 1) for i in range(16)])


def to_chip(value, dy, dx):
    pairs = []
    for y in range(2):
        for x in range(SIDE):
            for core in range(2):
                pairs.append((y * 8 + x * 2 + core, (y ^ dy) * 8 + (x + dx) % SIDE * 2 + core))
    return lax.ppermute(value, "bundle", pairs)


def pick(table, index):
    dims = lax.GatherDimensionNumbers(
        offset_dims=(),
        collapsed_slice_dims=(0,),
        start_index_map=(0,),
        operand_batching_dims=(1,),
        start_indices_batching_dims=(1,),
    )
    return lax.gather(
        table, index[..., None], dims, (1, 1), mode=lax.GatherScatterMode.PROMISE_IN_BOUNDS
    )


def count_below(values, table):
    top = table(31)
    group = jnp.where(values > jnp.broadcast_to(top[3:4], values.shape), 4, 0)
    group = jnp.where(values > pick(top, group + 1), group + 2, group)
    group = jnp.where(values > pick(top, group), group + 1, group)

    def at(o):
        return pick(table(o), group)

    b4 = values > at(15)
    b5 = values > jnp.where(b4, at(23), at(7))
    b6 = values > jnp.where(b4, jnp.where(b5, at(27), at(19)), jnp.where(b5, at(11), at(3)))

    def among(o):
        pairs = [jnp.where(b6, at(8 * i + 4 + o), at(8 * i + o)) for i in range(4)]
        return jnp.where(b4, jnp.where(b5, pairs[3], pairs[2]), jnp.where(b5, pairs[1], pairs[0]))

    b7 = values > among(1)
    b8 = values > jnp.where(b7, among(2), among(0))
    count = group * 32
    for bit, weight in ((b4, 16), (b5, 8), (b6, 4), (b7, 2), (b8, 1)):
        count = count + jnp.where(bit, weight, 0)
    return count


def prep_kernel(spot_ref, raw_ref, *refs):
    outs, buffer, sems, turned = refs[:CHIPS], refs[CHIPS], refs[CHIPS + 1], refs[CHIPS + 2 :]
    i = pl.program_id(0)

    def turn(j):
        flat = raw_ref[:, j * SUB : (j + 1) * SUB].T
        turned[j][pl.ds(0, SUB, stride=2), :] = flat[:, :128]
        turned[j][pl.ds(1, SUB, stride=2), :] = flat[:, 128:]

    def scatter(j):
        base = i * GROUP + j * SUB
        for start in range(0, SUB, 32):
            rows = []
            for q in range(8):
                four = turned[j][2 * start + 8 * q : 2 * start + 8 * q + 8, :]
                rows += [four[2 * k : 2 * k + 2, :] for k in range(4)]
            for k in range(32):
                buffer[spot_ref[base + start + k]] = rows[k]

    turn(0)
    for j in range(len(turned)):
        if j + 1 < len(turned):
            turn(j + 1)
        scatter(j)

    @pl.when(i == pl.num_programs(0) - 1)
    def _():
        copies = []
        for k, ref in enumerate(outs):
            copies.append(pltpu.make_async_copy(buffer.at[pl.ds(512 * k, 512)], ref, sems.at[k]))
        for copy in copies:
            copy.start()
        for copy in copies:
            copy.wait()


def prep(spot, raw):
    return pl.pallas_call(
        prep_kernel,
        grid_spec=pltpu.PrefetchScalarGridSpec(
            num_scalar_prefetch=1,
            grid=(FEATURES // GROUP,),
            in_specs=[pl.BlockSpec((256, GROUP), lambda i, c: (0, i))],
            out_specs=[pl.BlockSpec(memory_space=pltpu.HBM)] * CHIPS,
            scratch_shapes=[pltpu.VMEM((FEATURES, 2, 128), jnp.float32), pltpu.SemaphoreType.DMA((CHIPS,))]
            + [pltpu.VMEM((SUB * 2, 128), jnp.float32)] * (GROUP // SUB),
        ),
        out_shape=[jax.ShapeDtypeStruct((512, 2, 128), jnp.float32)] * CHIPS,
        name="prep",
    )(spot, raw)


def choose_kernel(row_ref, mine_ref, other_ref, out_ref, pool):
    pool[0:512, :] = mine_ref[...]
    pool[512:1024, :] = other_ref[...]
    pool[1024:1032, :] = jnp.zeros((8, EDGES), jnp.float32)

    def eight(i, carry):
        rows = [pool[pl.ds(row_ref[i * 8 + k], 1), :] for k in range(8)]
        out_ref[pl.ds(pl.multiple_of(i * 8, 8), 8), :] = jnp.concatenate(rows, axis=0)
        return carry

    lax.fori_loop(0, SPAN // 8, eight, 0)


def choose(row, mine, other):
    whole = pl.BlockSpec((512, EDGES), lambda i, r: (0, 0))
    return pl.pallas_call(
        choose_kernel,
        grid_spec=pltpu.PrefetchScalarGridSpec(
            num_scalar_prefetch=1,
            grid=(1,),
            in_specs=[whole, whole],
            out_specs=pl.BlockSpec((SPAN, EDGES), lambda i, r: (0, 0)),
            scratch_shapes=[pltpu.VMEM((1032, EDGES), jnp.float32)],
        ),
        out_shape=jax.ShapeDtypeStruct((SPAN, EDGES), jnp.float32),
        name="choose",
    )(row, mine, other)


def table_kernel(a_ref, b_ref, c_ref, d_ref, out_ref):
    total = (a_ref[...] + b_ref[...]) + (c_ref[...] + d_ref[...])
    out_ref[...] = total.T


def make_table(parts):
    return pl.pallas_call(
        table_kernel, out_shape=jax.ShapeDtypeStruct((EDGES, SPAN), jnp.float32), name="make_table"
    )(*parts)


def bin_kernel(row_ref, table_hbm, offset_ref, *refs, count, fresh, first):
    own, swapped = refs[:count], refs[count : 2 * count]
    out_ref, stage, turned, result, table_ref, in_sems, out_sems = refs[2 * count + (0 if fresh else 1) :]

    def take(i, side):
        source = own[i].at[0] if side == 0 else swapped[i].at[1]
        return pltpu.make_async_copy(source, stage.at[2 * i + side], in_sems.at[2 * i + side])

    def give(part):
        rows = pl.ds(pl.multiple_of(row_ref[first + part], 256), 256)
        return pltpu.make_async_copy(result.at[part], out_ref.at[rows, :], out_sems.at[part])

    tables = pltpu.make_async_copy(table_hbm, table_ref, in_sems.at[2 * count])
    for i in range(count):
        take(i, 0).start()
        if i == 0:
            tables.start()
        take(i, 1).start()

    def arrive(part):
        pltpu.make_async_copy(own[0].at[0], stage.at[part], in_sems.at[part]).wait()

    def turn(tile, slot):
        line = (tile % 4 // 2) * 256 + tile % 2
        turned[slot] = stage[tile // 4, pl.ds(line, 128, stride=2), :].T

    arrive(0)
    turn(0, 0)
    tables.wait()
    last = 8 * count - 1

    def one_tile(t, carry):
        following = jnp.minimum(t + 1, last)

        @pl.when((t % 4 == 3) & (t < last))
        def _():
            arrive(following // 4)

        lanes = pl.ds(pl.multiple_of((t % 4 // 2) * 128, 128), 128)
        offset = jnp.broadcast_to(offset_ref[:, lanes], (8, 128))
        for r in range(0, 128, 8):
            below = count_below(
                turned[t % 2, r : r + 8, :], lambda o: table_ref[8 * o : 8 * o + 8, lanes]
            )
            rows = pl.ds(pl.multiple_of((t % 2) * 128 + r, 8), 8)
            result[t // 4, rows, lanes] = below + offset
        turn(following, 1 - t % 2)

        @pl.when(t % 4 == 3)
        def _():
            give(t // 4).start()

        return carry

    lax.fori_loop(0, 8 * count, one_tile, 0)
    for part in range(2 * count):
        give(part).wait()


def bin_chips(row, first, table, offset, own, swapped, out):
    count, fresh = len(own), out is None
    anywhere = pl.BlockSpec(memory_space=pltpu.HBM)
    return pl.pallas_call(
        lambda *refs: bin_kernel(*refs, count=count, fresh=fresh, first=first),
        grid_spec=pltpu.PrefetchScalarGridSpec(
            num_scalar_prefetch=1,
            grid=(1,),
            in_specs=[
                anywhere,
                pl.BlockSpec((1, SPAN), lambda g, s: (0, 0)),
            ]
            + [anywhere] * (2 * count + (0 if fresh else 1)),
            out_specs=anywhere,
            scratch_shapes=[
                pltpu.VMEM((2 * count, 512, 128), jnp.float32),
                pltpu.VMEM((2, 128, 128), jnp.float32),
                pltpu.VMEM((2 * count, 256, SPAN), jnp.int32),
                pltpu.VMEM((EDGES, SPAN), jnp.float32),
                pltpu.SemaphoreType.DMA((2 * count + 1,)),
                pltpu.SemaphoreType.DMA((2 * count,)),
            ],
        ),
        out_shape=jax.ShapeDtypeStruct((16 * 256, SPAN), jnp.int32),
        input_output_aliases={} if fresh else {3 + 2 * count: 0},
    )(row, table, offset, *own, *swapped, *([] if fresh else [out]))


def step(raw_values, bin_edges, feature_column, bin_offset):
    row, bundle = lax.axis_index("rows"), lax.axis_index("bundle")
    z, core = row % SIDE, bundle % 2
    padded = jnp.pad(bin_edges, ((0, 0), (0, 1)))
    ordered = padded.reshape(PIECE, 8, 32).transpose(0, 2, 1).reshape(PIECE, EDGES)
    copies = jnp.broadcast_to(ordered[None], (16, PIECE, EDGES))
    mine = lax.all_to_all(copies, AXES, split_axis=0, concat_axis=0, axis_index_groups=planes(), tiled=True)
    mine = mine.reshape(512, EDGES)

    x, y_low = (bundle // 2) % SIDE, bundle // 8
    owner, inside = feature_column // SPAN, feature_column % SPAN
    chip = (owner // 8 ^ y_low) * SIDE + ((owner // 2) % SIDE - x) % SIDE
    spot = chip * 512 + (owner % 2 ^ core) * 256 + inside
    sent = [value.reshape(2, 512, 128) for value in prep(spot, raw_values)]

    def carry(chips, values):
        arrived = []
        for (dy, dx), value in zip(chips, values):
            arrived.append(to_chip(value, dy, dx))
        return arrived

    def picked(phase):
        return [sent[dy * SIDE + dx] for dy, dx in PHASES[phase]]

    arrived = [carry(PHASES[0], picked(0)), carry(PHASES[1], picked(1))]

    wanted = bundle * SPAN + jnp.arange(SPAN, dtype=jnp.int32)
    named = feature_column[None, :] == wanted[:, None]
    feature = jnp.max(jnp.where(named, jnp.arange(FEATURES, dtype=jnp.int32)[None], 0), axis=1)
    offset = jnp.max(jnp.where(named, bin_offset[None], 0), axis=1)
    device = feature // PIECE
    far_y = (device // 64) * 2 + (device // 8) % 2
    line = (far_y * SIDE + (device // 2) % SIDE) * PIECE + feature % PIECE
    line = jnp.where(device % 2 == core, line, line + 512)
    line = jnp.where((device // 16) % SIDE == z, line, 1024)
    part = choose(line, mine, swap_cores(mine))
    turned = []
    for step in (1, 3, 2):
        turned.append(along_z(part, step))
    for phase in (2, 3):
        *values, arrived[phase - 2] = lax.optimization_barrier((*picked(phase), arrived[phase - 2]))
        arrived.append(carry(PHASES[phase], values))
    table = make_table([part] + turned)
    groups = [((0, 0), *PHASES[0])] + list(PHASES[1:])
    arrived[0] = [sent[0]] + arrived[0]
    row = []
    for dy, dx in sum(map(tuple, groups), ()):
        base = ((y_low ^ dy) * SIDE + (x - dx) % SIDE) * 512
        row += [base + core * 256, base + (1 - core) * 256]
    row = jnp.stack(row).astype(jnp.int32)
    swapped = []
    for n in range(2):
        swapped.append([])
        for value in arrived[n]:
            swapped[n].append(swap_cores(value))
    out, first = None, 0
    for n in range(4):
        own, other = arrived[n], swapped[n]
        if n < 2:
            out = bin_chips(row, first, table, offset[None], own, other, out)
            arrived[n + 2], out = lax.optimization_barrier((arrived[n + 2], out))
            swapped.append([swap_cores(value) for value in arrived[n + 2]])
        else:
            out = bin_chips(row, first, table, offset[None], own, other, out)
        first += 2 * len(own)
    return out


def solution(mesh):
    in_specs = (P(AXES, None), P(AXES, None), P(), P())
    return jax.shard_map(step, mesh=mesh, in_specs=in_specs, out_specs=P("rows", "bundle"), check_vma=False)
```

```python
import jax
import jax.numpy as jnp
from jax import lax
from jax.experimental import pallas as pl
from jax.experimental.pallas import tpu as pltpu
from jax.sharding import PartitionSpec as P


AXES = ("rows", "bundle")
SIDE = 4
PIECE = 32
EDGES = 256
SPAN = 256
FEATURES = 4096
CHIPS = 8
PHASES = (((1, 0), (0, 2)), ((1, 1), (0, 3)), ((1, 3), (0, 1)), ((1, 2),))
GROUP = 1024
SUB = 256


def device_at(y, z, x, core):
    return ((y // 2) * 4 + z) * 16 + (y % 2) * 8 + x * 2 + core


def planes():
    ring = range(SIDE)
    return [[device_at(y, z, x, core) for y in ring for x in ring] for z in ring for core in range(2)]


def along_z(value, step):
    pairs = [(h * SIDE + (z + step) % SIDE, h * SIDE + z) for h in range(2) for z in range(SIDE)]
    return lax.ppermute(value, "rows", pairs)


def swap_cores(value):
    return lax.ppermute(value, "bundle", [(i, i ^ 1) for i in range(16)])


def to_chip(value, dy, dx):
    pairs = []
    for y in range(2):
        for x in range(SIDE):
            for core in range(2):
                pairs.append((y * 8 + x * 2 + core, (y ^ dy) * 8 + (x + dx) % SIDE * 2 + core))
    return lax.ppermute(value, "bundle", pairs)


def pick(table, index):
    dims = lax.GatherDimensionNumbers(
        offset_dims=(),
        collapsed_slice_dims=(0,),
        start_index_map=(0,),
        operand_batching_dims=(1,),
        start_indices_batching_dims=(1,),
    )
    return lax.gather(
        table, index[..., None], dims, (1, 1), mode=lax.GatherScatterMode.PROMISE_IN_BOUNDS
    )


def count_below(values, table):
    top = table(31)
    group = jnp.where(values > jnp.broadcast_to(top[3:4], values.shape), 4, 0)
    group = jnp.where(values > pick(top, group + 1), group + 2, group)
    group = jnp.where(values > pick(top, group), group + 1, group)

    def at(o):
        return pick(table(o), group)

    b4 = values > at(15)
    b5 = values > jnp.where(b4, at(23), at(7))
    b6 = values > jnp.where(b4, jnp.where(b5, at(27), at(19)), jnp.where(b5, at(11), at(3)))

    def among(o):
        pairs = [jnp.where(b6, at(8 * i + 4 + o), at(8 * i + o)) for i in range(4)]
        return jnp.where(b4, jnp.where(b5, pairs[3], pairs[2]), jnp.where(b5, pairs[1], pairs[0]))

    b7 = values > among(1)
    b8 = values > jnp.where(b7, among(2), among(0))
    count = group * 32
    for bit, weight in ((b4, 16), (b5, 8), (b6, 4), (b7, 2), (b8, 1)):
        count = count + jnp.where(bit, weight, 0)
    return count


def prep_kernel(spot_ref, raw_ref, *refs):
    outs, buffer, sems, turned = refs[:CHIPS], refs[CHIPS], refs[CHIPS + 1], refs[CHIPS + 2 :]
    i = pl.program_id(0)

    def turn(j):
        flat = raw_ref[:, j * SUB : (j + 1) * SUB].T
        turned[j][pl.ds(0, SUB, stride=2), :] = flat[:, :128]
        turned[j][pl.ds(1, SUB, stride=2), :] = flat[:, 128:]

    def scatter(j):
        base = i * GROUP + j * SUB
        for start in range(0, SUB, 32):
            rows = []
            for q in range(8):
                four = turned[j][2 * start + 8 * q : 2 * start + 8 * q + 8, :]
                rows += [four[2 * k : 2 * k + 2, :] for k in range(4)]
            for k in range(32):
                buffer[spot_ref[base + start + k]] = rows[k]

    turn(0)
    for j in range(len(turned)):
        if j + 1 < len(turned):
            turn(j + 1)
        scatter(j)

    @pl.when(i == pl.num_programs(0) - 1)
    def _():
        copies = []
        for k, ref in enumerate(outs):
            copies.append(pltpu.make_async_copy(buffer.at[pl.ds(512 * k, 512)], ref, sems.at[k]))
        for copy in copies:
            copy.start()
        for copy in copies:
            copy.wait()


def prep(spot, raw):
    return pl.pallas_call(
        prep_kernel,
        grid_spec=pltpu.PrefetchScalarGridSpec(
            num_scalar_prefetch=1,
            grid=(FEATURES // GROUP,),
            in_specs=[pl.BlockSpec((256, GROUP), lambda i, c: (0, i))],
            out_specs=[pl.BlockSpec(memory_space=pltpu.HBM)] * CHIPS,
            scratch_shapes=[pltpu.VMEM((FEATURES, 2, 128), jnp.float32), pltpu.SemaphoreType.DMA((CHIPS,))]
            + [pltpu.VMEM((SUB * 2, 128), jnp.float32)] * (GROUP // SUB),
        ),
        out_shape=[jax.ShapeDtypeStruct((512, 2, 128), jnp.float32)] * CHIPS,
        name="prep",
    )(spot, raw)


def choose_kernel(row_ref, mine_ref, other_ref, out_ref, pool):
    pool[0:512, :] = mine_ref[...]
    pool[512:1024, :] = other_ref[...]
    pool[1024:1032, :] = jnp.zeros((8, EDGES), jnp.float32)

    def eight(i, carry):
        rows = [pool[pl.ds(row_ref[i * 8 + k], 1), :] for k in range(8)]
        out_ref[pl.ds(pl.multiple_of(i * 8, 8), 8), :] = jnp.concatenate(rows, axis=0)
        return carry

    lax.fori_loop(0, SPAN // 8, eight, 0)


def choose(row, mine, other):
    whole = pl.BlockSpec((512, EDGES), lambda i, r: (0, 0))
    return pl.pallas_call(
        choose_kernel,
        grid_spec=pltpu.PrefetchScalarGridSpec(
            num_scalar_prefetch=1,
            grid=(1,),
            in_specs=[whole, whole],
            out_specs=pl.BlockSpec((SPAN, EDGES), lambda i, r: (0, 0)),
            scratch_shapes=[pltpu.VMEM((1032, EDGES), jnp.float32)],
        ),
        out_shape=jax.ShapeDtypeStruct((SPAN, EDGES), jnp.float32),
        name="choose",
    )(row, mine, other)


def table_kernel(a_ref, b_ref, c_ref, d_ref, offset_ref, out_ref):
    total = (a_ref[...] + b_ref[...]) + (c_ref[...] + d_ref[...])
    turned = total.T
    line = lax.broadcasted_iota(jnp.int32, turned.shape, 0)
    out_ref[...] = jnp.where(line == EDGES - 1, offset_ref[...].astype(jnp.float32), turned)


def make_table(parts, offset):
    return pl.pallas_call(
        table_kernel, out_shape=jax.ShapeDtypeStruct((EDGES, SPAN), jnp.float32), name="make_table"
    )(*parts, offset)


def bin_kernel(table_hbm, *refs, chips, fresh):
    count = len(chips)
    own, swapped = refs[:count], refs[count : 2 * count]
    bundle = lax.axis_index("bundle")
    x, y_low, core = (bundle // 2) % SIDE, bundle // 8, bundle % 2
    out_ref, stage, turned, result, table_ref, bases, in_sems, out_sems = refs[2 * count + (0 if fresh else 1) :]

    def take(i, side):
        source = own[i].at[0] if side == 0 else swapped[i].at[1]
        return pltpu.make_async_copy(source, stage.at[2 * i + side], in_sems.at[2 * i + side])

    for i, (dy, dx) in enumerate(chips):
        base = (jnp.where(y_low == dy, 0, SIDE) + (x - dx + SIDE) % SIDE) * 512
        bases[2 * i] = base + core * 256
        bases[2 * i + 1] = base + (1 - core) * 256

    def give(tile):
        part = tile // 4
        rows = pl.ds(pl.multiple_of(bases[part] + (tile % 2) * 128, 128), 128)
        lanes = pl.ds(pl.multiple_of((tile % 4 // 2) * 128, 128), 128)
        return pltpu.make_async_copy(result.at[tile], out_ref.at[rows, lanes], out_sems.at[tile])

    tables = pltpu.make_async_copy(table_hbm, table_ref, in_sems.at[2 * count])
    for i in range(count):
        take(i, 0).start()
        if i == 0:
            tables.start()
        take(i, 1).start()

    def arrive(part):
        pltpu.make_async_copy(own[0].at[0], stage.at[part], in_sems.at[part]).wait()

    def turn(tile, slot):
        line = (tile % 4 // 2) * 256 + tile % 2
        turned[slot] = stage[tile // 4, pl.ds(line, 128, stride=2), :].T

    arrive(0)
    turn(0, 0)
    tables.wait()
    last = 8 * count - 1

    def one_tile(t, carry):
        following = jnp.minimum(t + 1, last)

        @pl.when((t % 4 == 3) & (t < last))
        def _():
            arrive(following // 4)

        lanes = pl.ds(pl.multiple_of((t % 4 // 2) * 128, 128), 128)
        offset = jnp.broadcast_to(table_ref[EDGES - 1 :, lanes].astype(jnp.int32), (8, 128))
        for r in range(0, 128, 8):
            below = count_below(
                turned[t % 2, r : r + 8, :], lambda o: table_ref[8 * o : 8 * o + 8, lanes]
            )
            result[t, r : r + 8, :] = below + offset
        turn(following, 1 - t % 2)
        give(t).start()
        return carry

    lax.fori_loop(0, 8 * count, one_tile, 0)

    def drain(t, carry):
        give(t).wait()
        return carry

    lax.fori_loop(0, 8 * count, drain, 0)


def bin_chips(chips, table, own, swapped, out):
    count, fresh = len(own), out is None
    anywhere = pl.BlockSpec(memory_space=pltpu.HBM)
    return pl.pallas_call(
        lambda *refs: bin_kernel(*refs, chips=chips, fresh=fresh),
        in_specs=[anywhere] * (1 + 2 * count + (0 if fresh else 1)),
        out_specs=anywhere,
        scratch_shapes=[
            pltpu.VMEM((2 * count, 512, 128), jnp.float32),
            pltpu.VMEM((2, 128, 128), jnp.float32),
            pltpu.VMEM((8 * count, 128, 128), jnp.int32),
            pltpu.VMEM((EDGES, SPAN), jnp.float32),
            pltpu.SMEM((2 * count,), jnp.int32),
            pltpu.SemaphoreType.DMA((2 * count + 1,)),
            pltpu.SemaphoreType.DMA((8 * count,)),
        ],
        out_shape=jax.ShapeDtypeStruct((16 * 256, SPAN), jnp.int32),
        input_output_aliases={} if fresh else {1 + 2 * count: 0},
    )(table, *own, *swapped, *([] if fresh else [out]))


def step(raw_values, bin_edges, feature_column, bin_offset):
    row, bundle = lax.axis_index("rows"), lax.axis_index("bundle")
    z, core = row % SIDE, bundle % 2
    padded = jnp.pad(bin_edges, ((0, 0), (0, 1)))
    ordered = padded.reshape(PIECE, 8, 32).transpose(0, 2, 1).reshape(PIECE, EDGES)
    copies = jnp.broadcast_to(ordered[None], (16, PIECE, EDGES))
    mine = lax.all_to_all(copies, AXES, split_axis=0, concat_axis=0, axis_index_groups=planes(), tiled=True)
    mine = mine.reshape(512, EDGES)

    x, y_low = (bundle // 2) % SIDE, bundle // 8
    owner, inside = feature_column // SPAN, feature_column % SPAN
    chip = (owner // 8 ^ y_low) * SIDE + ((owner // 2) % SIDE - x) % SIDE
    spot = chip * 512 + (owner % 2 ^ core) * 256 + inside
    sent = [value.reshape(2, 512, 128) for value in prep(spot, raw_values)]

    def carry(chips, values):
        arrived = []
        for (dy, dx), value in zip(chips, values):
            arrived.append(to_chip(value, dy, dx))
        return arrived

    def picked(phase):
        return [sent[dy * SIDE + dx] for dy, dx in PHASES[phase]]

    arrived = [carry(PHASES[0], picked(0)), carry(PHASES[1], picked(1))]

    wanted = bundle * SPAN + jnp.arange(SPAN, dtype=jnp.int32)
    named = feature_column[None, :] == wanted[:, None]
    feature = jnp.max(jnp.where(named, jnp.arange(FEATURES, dtype=jnp.int32)[None], 0), axis=1)
    offset = jnp.max(jnp.where(named, bin_offset[None], 0), axis=1)
    device = feature // PIECE
    far_y = (device // 64) * 2 + (device // 8) % 2
    line = (far_y * SIDE + (device // 2) % SIDE) * PIECE + feature % PIECE
    line = jnp.where(device % 2 == core, line, line + 512)
    line = jnp.where((device // 16) % SIDE == z, line, 1024)
    part = choose(line, mine, swap_cores(mine))
    turned = []
    for step in (1, 3, 2):
        turned.append(along_z(part, step))
    arrived.append(carry(PHASES[2], picked(2)))
    *values, arrived[1] = lax.optimization_barrier((*picked(3), arrived[1]))
    arrived.append(carry(PHASES[3], values))
    table = make_table([part] + turned, offset[None])
    arrived[0] = [sent[0]] + arrived[0]
    chips = [((0, 0), *PHASES[0])] + list(PHASES[1:])
    swapped = []
    for n in range(2):
        swapped.append([])
        for value in arrived[n]:
            swapped[n].append(swap_cores(value))
    out = bin_chips(chips[0] + chips[1], table, arrived[0] + arrived[1], swapped[0] + swapped[1], None)
    for n in (2, 3):
        arrived[n], out = lax.optimization_barrier((arrived[n], out))
        swapped.append([swap_cores(value) for value in arrived[n]])
        out = bin_chips(chips[n], table, arrived[n], swapped[n], out)
    return out


def solution(mesh):
    in_specs = (P(AXES, None), P(AXES, None), P(), P())
    return jax.shard_map(step, mesh=mesh, in_specs=in_specs, out_specs=P("rows", "bundle"), check_vma=False)
```

```python
import jax
import jax.numpy as jnp
from jax import lax
from jax.experimental import pallas as pl
from jax.experimental.pallas import tpu as pltpu
from jax.sharding import PartitionSpec as P


AXES = ("rows", "bundle")
SIDE = 4
PIECE = 32
EDGES = 256
SPAN = 256
FEATURES = 4096
EARLY = ((1, 0), (0, 2), (1, 1), (0, 3))
LATE = ((1, 3), (0, 1), (1, 2))
GROUP = 1024
SUB = 256


CUTS = [((dy * SIDE + dx) * 512, 512) for dy, dx in ((0, 0), *EARLY)]
CUTS += [((dy * SIDE + dx) * 512 + dc * 256, 256) for dy, dx in LATE for dc in range(2)]


def device_at(y, z, x, core):
    return ((y // 2) * 4 + z) * 16 + (y % 2) * 8 + x * 2 + core


def planes():
    ring = range(SIDE)
    return [[device_at(y, z, x, core) for y in ring for x in ring] for z in ring for core in range(2)]


def along_z(value, step):
    pairs = [(h * SIDE + (z + step) % SIDE, h * SIDE + z) for h in range(2) for z in range(SIDE)]
    return lax.ppermute(value, "rows", pairs)


def swap_cores(value):
    return lax.ppermute(value, "bundle", [(i, i ^ 1) for i in range(16)])


def to_chip(value, dy, dx, dc=0):
    pairs = []
    for y in range(2):
        for x in range(SIDE):
            for core in range(2):
                pairs.append((y * 8 + x * 2 + core, (y ^ dy) * 8 + (x + dx) % SIDE * 2 + (core ^ dc)))
    return lax.ppermute(value, "bundle", pairs)


def pick(table, index):
    dims = lax.GatherDimensionNumbers(
        offset_dims=(),
        collapsed_slice_dims=(0,),
        start_index_map=(0,),
        operand_batching_dims=(1,),
        start_indices_batching_dims=(1,),
    )
    return lax.gather(
        table, index[..., None], dims, (1, 1), mode=lax.GatherScatterMode.PROMISE_IN_BOUNDS
    )


def count_below(values, table):
    top = table(31)
    group = jnp.where(values > jnp.broadcast_to(top[3:4], values.shape), 4, 0)
    group = jnp.where(values > pick(top, group + 1), group + 2, group)
    group = jnp.where(values > pick(top, group), group + 1, group)

    def at(o):
        return pick(table(o), group)

    b4 = values > at(15)
    b5 = values > jnp.where(b4, at(23), at(7))
    b6 = values > jnp.where(b4, jnp.where(b5, at(27), at(19)), jnp.where(b5, at(11), at(3)))

    def among(o):
        pairs = [jnp.where(b6, at(8 * i + 4 + o), at(8 * i + o)) for i in range(4)]
        return jnp.where(b4, jnp.where(b5, pairs[3], pairs[2]), jnp.where(b5, pairs[1], pairs[0]))

    b7 = values > among(1)
    b8 = values > jnp.where(b7, among(2), among(0))
    count = group * 32
    for bit, weight in ((b4, 16), (b5, 8), (b6, 4), (b7, 2), (b8, 1)):
        count = count + jnp.where(bit, weight, 0)
    return count


def prep_kernel(spot_ref, raw_ref, *refs):
    outs = refs[: len(CUTS)]
    buffer, sems, *turned = refs[len(CUTS) :]
    i = pl.program_id(0)

    def turn(j):
        flat = raw_ref[:, j * SUB : (j + 1) * SUB].T
        turned[j][pl.ds(0, SUB, stride=2), :] = flat[:, :128]
        turned[j][pl.ds(1, SUB, stride=2), :] = flat[:, 128:]

    def scatter(j):
        base = i * GROUP + j * SUB
        for start in range(0, SUB, 32):
            rows = []
            for q in range(8):
                four = turned[j][2 * start + 8 * q : 2 * start + 8 * q + 8, :]
                rows += [four[2 * k : 2 * k + 2, :] for k in range(4)]
            for k in range(32):
                buffer[spot_ref[base + start + k]] = rows[k]

    turn(0)
    for j in range(len(turned)):
        if j + 1 < len(turned):
            turn(j + 1)
        scatter(j)

    @pl.when(i == pl.num_programs(0) - 1)
    def _():
        copies = []
        for k, (ref, (start, size)) in enumerate(zip(outs, CUTS)):
            copies.append(pltpu.make_async_copy(buffer.at[pl.ds(start, size)], ref, sems.at[k]))
        for copy in copies:
            copy.start()
        for copy in copies:
            copy.wait()


def prep(spot, raw):
    return pl.pallas_call(
        prep_kernel,
        grid_spec=pltpu.PrefetchScalarGridSpec(
            num_scalar_prefetch=1,
            grid=(FEATURES // GROUP,),
            in_specs=[pl.BlockSpec((256, GROUP), lambda i, c: (0, i))],
            out_specs=[pl.BlockSpec(memory_space=pltpu.HBM)] * len(CUTS),
            scratch_shapes=[pltpu.VMEM((FEATURES, 2, 128), jnp.float32), pltpu.SemaphoreType.DMA((len(CUTS),))]
            + [pltpu.VMEM((SUB * 2, 128), jnp.float32)] * (GROUP // SUB),
        ),
        out_shape=[jax.ShapeDtypeStruct((size, 2, 128), jnp.float32) for _, size in CUTS],
        name="prep",
    )(spot, raw)


def choose_kernel(row_ref, mine_ref, other_ref, out_ref, pool):
    pool[0:512, :] = mine_ref[...]
    pool[512:1024, :] = other_ref[...]
    pool[1024:1032, :] = jnp.zeros((8, EDGES), jnp.float32)

    def eight(i, carry):
        rows = [pool[pl.ds(row_ref[i * 8 + k], 1), :] for k in range(8)]
        out_ref[pl.ds(pl.multiple_of(i * 8, 8), 8), :] = jnp.concatenate(rows, axis=0)
        return carry

    lax.fori_loop(0, SPAN // 8, eight, 0)


def choose(row, mine, other):
    whole = pl.BlockSpec((512, EDGES), lambda i, r: (0, 0))
    return pl.pallas_call(
        choose_kernel,
        grid_spec=pltpu.PrefetchScalarGridSpec(
            num_scalar_prefetch=1,
            grid=(1,),
            in_specs=[whole, whole],
            out_specs=pl.BlockSpec((SPAN, EDGES), lambda i, r: (0, 0)),
            scratch_shapes=[pltpu.VMEM((1032, EDGES), jnp.float32)],
        ),
        out_shape=jax.ShapeDtypeStruct((SPAN, EDGES), jnp.float32),
        name="choose",
    )(row, mine, other)


def table_kernel(a_ref, b_ref, c_ref, d_ref, offset_ref, out_ref):
    total = (a_ref[...] + b_ref[...]) + (c_ref[...] + d_ref[...])
    turned = total.T
    line = lax.broadcasted_iota(jnp.int32, turned.shape, 0)
    out_ref[...] = jnp.where(line == EDGES - 1, offset_ref[...].astype(jnp.float32), turned)


def make_table(parts, offset):
    return pl.pallas_call(
        table_kernel, out_shape=jax.ShapeDtypeStruct((EDGES, SPAN), jnp.float32), name="make_table"
    )(*parts, offset)


def bin_kernel(table_hbm, *refs, chips, fresh):
    count = len(chips)
    parts = refs[: 2 * count]
    bundle = lax.axis_index("bundle")
    x, y_low, core = (bundle // 2) % SIDE, bundle // 8, bundle % 2
    out_ref, stage, turned, result, table_ref, bases, in_sems, out_sems = refs[2 * count + (0 if fresh else 1) :]

    def take(i, side):
        source = parts[2 * i + side]
        source = source.at[side] if len(source.shape) == 3 else source
        return pltpu.make_async_copy(source, stage.at[2 * i + side], in_sems.at[2 * i + side])

    for i, (dy, dx) in enumerate(chips):
        base = (jnp.where(y_low == dy, 0, SIDE) + (x - dx + SIDE) % SIDE) * 512
        bases[2 * i] = base + core * 256
        bases[2 * i + 1] = base + (1 - core) * 256

    def give(tile):
        part = tile // 4
        rows = pl.ds(pl.multiple_of(bases[part] + (tile % 2) * 128, 128), 128)
        lanes = pl.ds(pl.multiple_of((tile % 4 // 2) * 128, 128), 128)
        return pltpu.make_async_copy(result.at[tile], out_ref.at[rows, lanes], out_sems.at[tile])

    tables = pltpu.make_async_copy(table_hbm, table_ref, in_sems.at[2 * count])
    for i in range(count):
        take(i, 0).start()
        if i == 0:
            tables.start()
        take(i, 1).start()

    def arrive(part):
        pltpu.make_async_copy(stage.at[0], stage.at[part], in_sems.at[part]).wait()

    def turn(tile, slot):
        line = (tile % 4 // 2) * 256 + tile % 2
        turned[slot] = stage[tile // 4, pl.ds(line, 128, stride=2), :].T

    arrive(0)
    turn(0, 0)
    tables.wait()
    last = 8 * count - 1

    def one_tile(t, carry):
        following = jnp.minimum(t + 1, last)

        @pl.when((t % 4 == 3) & (t < last))
        def _():
            arrive(following // 4)

        lanes = pl.ds(pl.multiple_of((t % 4 // 2) * 128, 128), 128)
        offset = jnp.broadcast_to(table_ref[EDGES - 1 :, lanes].astype(jnp.int32), (8, 128))
        for r in range(0, 128, 8):
            below = count_below(
                turned[t % 2, r : r + 8, :], lambda o: table_ref[8 * o : 8 * o + 8, lanes]
            )
            result[t, r : r + 8, :] = below + offset
        turn(following, 1 - t % 2)
        give(t).start()
        return carry

    lax.fori_loop(0, 8 * count, one_tile, 0)

    def drain(t, carry):
        give(t).wait()
        return carry

    lax.fori_loop(0, 8 * count, drain, 0)


def bin_chips(chips, table, parts, out):
    count, fresh = len(chips), out is None
    anywhere = pl.BlockSpec(memory_space=pltpu.HBM)
    return pl.pallas_call(
        lambda *refs: bin_kernel(*refs, chips=chips, fresh=fresh),
        in_specs=[anywhere] * (1 + 2 * count + (0 if fresh else 1)),
        out_specs=anywhere,
        scratch_shapes=[
            pltpu.VMEM((2 * count, 512, 128), jnp.float32),
            pltpu.VMEM((2, 128, 128), jnp.float32),
            pltpu.VMEM((8 * count, 128, 128), jnp.int32),
            pltpu.VMEM((EDGES, SPAN), jnp.float32),
            pltpu.SMEM((2 * count,), jnp.int32),
            pltpu.SemaphoreType.DMA((2 * count + 1,)),
            pltpu.SemaphoreType.DMA((8 * count,)),
        ],
        out_shape=jax.ShapeDtypeStruct((16 * 256, SPAN), jnp.int32),
        input_output_aliases={} if fresh else {1 + 2 * count: 0},
    )(table, *parts, *([] if fresh else [out]))


def step(raw_values, bin_edges, feature_column, bin_offset):
    row, bundle = lax.axis_index("rows"), lax.axis_index("bundle")
    z, core = row % SIDE, bundle % 2
    padded = jnp.pad(bin_edges, ((0, 0), (0, 1)))
    ordered = padded.reshape(PIECE, 8, 32).transpose(0, 2, 1).reshape(PIECE, EDGES)
    copies = jnp.broadcast_to(ordered[None], (16, PIECE, EDGES))
    mine = lax.all_to_all(copies, AXES, split_axis=0, concat_axis=0, axis_index_groups=planes(), tiled=True)
    mine = mine.reshape(512, EDGES)

    x, y_low = (bundle // 2) % SIDE, bundle // 8
    owner, inside = feature_column // SPAN, feature_column % SPAN
    chip = (owner // 8 ^ y_low) * SIDE + ((owner // 2) % SIDE - x) % SIDE
    spot = chip * 512 + (owner % 2 ^ core) * 256 + inside
    pieces = prep(spot, raw_values)
    sent = [value.reshape(2, 512, 128) for value in pieces[: 1 + len(EARLY)]]
    halves = [value.reshape(512, 128) for value in pieces[1 + len(EARLY) :]]
    arrived = [sent[0]]
    for (dy, dx), value in zip(EARLY, sent[1:]):
        arrived.append(to_chip(value, dy, dx))
    direct = []
    for i, (dy, dx) in enumerate(LATE):
        for dc in range(2):
            direct.append(to_chip(halves[2 * i + dc], dy, dx, dc))

    wanted = bundle * SPAN + jnp.arange(SPAN, dtype=jnp.int32)
    named = feature_column[None, :] == wanted[:, None]
    feature = jnp.max(jnp.where(named, jnp.arange(FEATURES, dtype=jnp.int32)[None], 0), axis=1)
    offset = jnp.max(jnp.where(named, bin_offset[None], 0), axis=1)
    device = feature // PIECE
    far_y = (device // 64) * 2 + (device // 8) % 2
    line = (far_y * SIDE + (device // 2) % SIDE) * PIECE + feature % PIECE
    line = jnp.where(device % 2 == core, line, line + 512)
    line = jnp.where((device // 16) % SIDE == z, line, 1024)
    part = choose(line, mine, swap_cores(mine))
    turned = []
    for step in (1, 3, 2):
        turned.append(along_z(part, step))
    table = make_table([part] + turned, offset[None])
    parts = []
    for value in arrived:
        parts += [value, swap_cores(value)]
    out = bin_chips(((0, 0), *EARLY), table, parts, None)
    *direct, out = lax.optimization_barrier((*direct, out))
    return bin_chips(LATE, table, direct, out)


def solution(mesh):
    in_specs = (P(AXES, None), P(AXES, None), P(), P())
    return jax.shard_map(step, mesh=mesh, in_specs=in_specs, out_specs=P("rows", "bundle"), check_vma=False)
```

```python
import jax
import jax.numpy as jnp
from jax import lax
from jax.experimental import pallas as pl
from jax.experimental.pallas import tpu as pltpu
from jax.sharding import PartitionSpec as P


AXES = ("rows", "bundle")
SIDE = 4
PIECE = 32
EDGES = 256
SPAN = 256
FEATURES = 4096
EARLY = ((1, 0), (0, 2), (1, 1), (0, 3))
LATE = ((0, 1), (1, 3), (1, 2))
GROUP = 1024
SUB = 256


CUTS = [((dy * SIDE + dx) * 512, 512) for dy, dx in ((0, 0), *EARLY)]
CUTS += [((dy * SIDE + dx) * 512 + dc * 256, 256) for dy, dx in LATE for dc in range(2)]


def device_at(y, z, x, core):
    return ((y // 2) * 4 + z) * 16 + (y % 2) * 8 + x * 2 + core


def planes():
    ring = range(SIDE)
    return [[device_at(y, z, x, core) for y in ring for x in ring] for z in ring for core in range(2)]


def along_z(value, step):
    pairs = [(h * SIDE + (z + step) % SIDE, h * SIDE + z) for h in range(2) for z in range(SIDE)]
    return lax.ppermute(value, "rows", pairs)


def swap_cores(value):
    return lax.ppermute(value, "bundle", [(i, i ^ 1) for i in range(16)])


def to_chip(value, dy, dx, dc=0):
    pairs = []
    for y in range(2):
        for x in range(SIDE):
            for core in range(2):
                pairs.append((y * 8 + x * 2 + core, (y ^ dy) * 8 + (x + dx) % SIDE * 2 + (core ^ dc)))
    return lax.ppermute(value, "bundle", pairs)


def pick(table, index):
    dims = lax.GatherDimensionNumbers(
        offset_dims=(),
        collapsed_slice_dims=(0,),
        start_index_map=(0,),
        operand_batching_dims=(1,),
        start_indices_batching_dims=(1,),
    )
    return lax.gather(
        table, index[..., None], dims, (1, 1), mode=lax.GatherScatterMode.PROMISE_IN_BOUNDS
    )


def count_below(values, table):
    top = table(31)
    group = jnp.where(values > jnp.broadcast_to(top[3:4], values.shape), 4, 0)
    group = jnp.where(values > pick(top, group + 1), group + 2, group)
    group = jnp.where(values > pick(top, group), group + 1, group)

    def at(o):
        return pick(table(o), group)

    b4 = values > at(15)
    b5 = values > jnp.where(b4, at(23), at(7))
    b6 = values > jnp.where(b4, jnp.where(b5, at(27), at(19)), jnp.where(b5, at(11), at(3)))

    def among(o):
        pairs = [jnp.where(b6, at(8 * i + 4 + o), at(8 * i + o)) for i in range(4)]
        return jnp.where(b4, jnp.where(b5, pairs[3], pairs[2]), jnp.where(b5, pairs[1], pairs[0]))

    b7 = values > among(1)
    b8 = values > jnp.where(b7, among(2), among(0))
    count = group * 32
    for bit, weight in ((b4, 16), (b5, 8), (b6, 4), (b7, 2), (b8, 1)):
        count = count + jnp.where(bit, weight, 0)
    return count


def prep_kernel(spot_ref, raw_ref, *refs):
    outs = refs[: len(CUTS)]
    buffer, sems, *turned = refs[len(CUTS) :]
    i = pl.program_id(0)

    def turn(j):
        flat = raw_ref[:, j * SUB : (j + 1) * SUB].T
        turned[j][pl.ds(0, SUB, stride=2), :] = flat[:, :128]
        turned[j][pl.ds(1, SUB, stride=2), :] = flat[:, 128:]

    def scatter(j):
        base = i * GROUP + j * SUB
        for start in range(0, SUB, 32):
            rows = []
            for q in range(8):
                four = turned[j][2 * start + 8 * q : 2 * start + 8 * q + 8, :]
                rows += [four[2 * k : 2 * k + 2, :] for k in range(4)]
            for k in range(32):
                buffer[spot_ref[base + start + k]] = rows[k]

    turn(0)
    for j in range(len(turned)):
        if j + 1 < len(turned):
            turn(j + 1)
        scatter(j)

    @pl.when(i == pl.num_programs(0) - 1)
    def _():
        copies = []
        for k, (ref, (start, size)) in enumerate(zip(outs, CUTS)):
            copies.append(pltpu.make_async_copy(buffer.at[pl.ds(start, size)], ref, sems.at[k]))
        for copy in copies:
            copy.start()
        for copy in copies:
            copy.wait()


def prep(spot, raw):
    return pl.pallas_call(
        prep_kernel,
        grid_spec=pltpu.PrefetchScalarGridSpec(
            num_scalar_prefetch=1,
            grid=(FEATURES // GROUP,),
            in_specs=[pl.BlockSpec((256, GROUP), lambda i, c: (0, i))],
            out_specs=[pl.BlockSpec(memory_space=pltpu.HBM)] * len(CUTS),
            scratch_shapes=[pltpu.VMEM((FEATURES, 2, 128), jnp.float32), pltpu.SemaphoreType.DMA((len(CUTS),))]
            + [pltpu.VMEM((SUB * 2, 128), jnp.float32)] * (GROUP // SUB),
        ),
        out_shape=[jax.ShapeDtypeStruct((size, 2, 128), jnp.float32) for _, size in CUTS],
        name="prep",
    )(spot, raw)


def choose_kernel(row_ref, mine_ref, other_ref, out_ref, pool):
    pool[0:512, :] = mine_ref[...]
    pool[512:1024, :] = other_ref[...]
    pool[1024:1032, :] = jnp.zeros((8, EDGES), jnp.float32)

    def eight(i, carry):
        rows = [pool[pl.ds(row_ref[i * 8 + k], 1), :] for k in range(8)]
        out_ref[pl.ds(pl.multiple_of(i * 8, 8), 8), :] = jnp.concatenate(rows, axis=0)
        return carry

    lax.fori_loop(0, SPAN // 8, eight, 0)


def choose(row, mine, other):
    whole = pl.BlockSpec((512, EDGES), lambda i, r: (0, 0))
    return pl.pallas_call(
        choose_kernel,
        grid_spec=pltpu.PrefetchScalarGridSpec(
            num_scalar_prefetch=1,
            grid=(1,),
            in_specs=[whole, whole],
            out_specs=pl.BlockSpec((SPAN, EDGES), lambda i, r: (0, 0)),
            scratch_shapes=[pltpu.VMEM((1032, EDGES), jnp.float32)],
        ),
        out_shape=jax.ShapeDtypeStruct((SPAN, EDGES), jnp.float32),
        name="choose",
    )(row, mine, other)


def table_kernel(a_ref, b_ref, c_ref, d_ref, offset_ref, out_ref, turned):
    total = (a_ref[...] + b_ref[...]) + (c_ref[...] + d_ref[...])
    for half in range(2):
        turned[half] = total[half * 128 : half * 128 + 128, :].T
    for o in range(32):
        for half in range(2):
            lanes = slice(half * 128, half * 128 + 128)
            out_ref[8 * o : 8 * o + 8, lanes] = turned[half, pl.ds(o, 8, stride=32), :]
    out_ref[EDGES - 1 :, :] = offset_ref[...].astype(jnp.float32)


def make_table(parts, offset):
    return pl.pallas_call(
        table_kernel,
        out_shape=jax.ShapeDtypeStruct((EDGES, SPAN), jnp.float32),
        scratch_shapes=[pltpu.VMEM((2, EDGES, 128), jnp.float32)],
        name="make_table",
    )(*parts, offset)


def bin_kernel(table_hbm, *refs, chips, fresh):
    count = len(chips)
    parts = refs[: 2 * count]
    bundle = lax.axis_index("bundle")
    x, y_low, core = (bundle // 2) % SIDE, bundle // 8, bundle % 2
    out_ref, stage, turned, result, table_ref, bases, in_sems, out_sems = refs[2 * count + (0 if fresh else 1) :]

    def take(i, side):
        source = parts[2 * i + side]
        source = source.at[side] if len(source.shape) == 3 else source
        return pltpu.make_async_copy(source, stage.at[2 * i + side], in_sems.at[2 * i + side])

    for i, (dy, dx) in enumerate(chips):
        base = (jnp.where(y_low == dy, 0, SIDE) + (x - dx + SIDE) % SIDE) * 512
        bases[2 * i] = base + core * 256
        bases[2 * i + 1] = base + (1 - core) * 256

    def give(tile):
        part = tile // 4
        rows = pl.ds(pl.multiple_of(bases[part] + (tile % 2) * 128, 128), 128)
        lanes = pl.ds(pl.multiple_of((tile % 4 // 2) * 128, 128), 128)
        return pltpu.make_async_copy(result.at[tile], out_ref.at[rows, lanes], out_sems.at[tile])

    tables = pltpu.make_async_copy(table_hbm, table_ref, in_sems.at[2 * count])
    for i in range(count):
        take(i, 0).start()
        if i == 0:
            tables.start()
        take(i, 1).start()

    def arrive(part):
        pltpu.make_async_copy(stage.at[0], stage.at[part], in_sems.at[part]).wait()

    def turn(tile, slot):
        line = (tile % 4 // 2) * 256 + tile % 2
        turned[slot] = stage[tile // 4, pl.ds(line, 128, stride=2), :].T

    arrive(0)
    turn(0, 0)
    tables.wait()
    last = 8 * count - 1

    def one_tile(t, carry):
        following = jnp.minimum(t + 1, last)

        @pl.when((t % 4 == 3) & (t < last))
        def _():
            arrive(following // 4)

        lanes = pl.ds(pl.multiple_of((t % 4 // 2) * 128, 128), 128)
        offset = jnp.broadcast_to(table_ref[EDGES - 1 :, lanes].astype(jnp.int32), (8, 128))
        for r in range(0, 128, 8):
            below = count_below(
                turned[t % 2, r : r + 8, :], lambda o: table_ref[8 * o : 8 * o + 8, lanes]
            )
            result[t, r : r + 8, :] = below + offset
        turn(following, 1 - t % 2)
        give(t).start()
        return carry

    lax.fori_loop(0, 8 * count, one_tile, 0)

    def drain(t, carry):
        give(t).wait()
        return carry

    lax.fori_loop(0, 8 * count, drain, 0)


def bin_chips(chips, table, parts, out):
    count, fresh = len(chips), out is None
    anywhere = pl.BlockSpec(memory_space=pltpu.HBM)
    return pl.pallas_call(
        lambda *refs: bin_kernel(*refs, chips=chips, fresh=fresh),
        in_specs=[anywhere] * (1 + 2 * count + (0 if fresh else 1)),
        out_specs=anywhere,
        scratch_shapes=[
            pltpu.VMEM((2 * count, 512, 128), jnp.float32),
            pltpu.VMEM((2, 128, 128), jnp.float32),
            pltpu.VMEM((8 * count, 128, 128), jnp.int32),
            pltpu.VMEM((EDGES, SPAN), jnp.float32),
            pltpu.SMEM((2 * count,), jnp.int32),
            pltpu.SemaphoreType.DMA((2 * count + 1,)),
            pltpu.SemaphoreType.DMA((8 * count,)),
        ],
        out_shape=jax.ShapeDtypeStruct((16 * 256, SPAN), jnp.int32),
        input_output_aliases={} if fresh else {1 + 2 * count: 0},
    )(table, *parts, *([] if fresh else [out]))


def step(raw_values, bin_edges, feature_column, bin_offset):
    row, bundle = lax.axis_index("rows"), lax.axis_index("bundle")
    z, core = row % SIDE, bundle % 2
    x, y_low = (bundle // 2) % SIDE, bundle // 8
    owner, inside = feature_column // SPAN, feature_column % SPAN
    chip = (owner // 8 ^ y_low) * SIDE + ((owner // 2) % SIDE - x) % SIDE
    spot = chip * 512 + (owner % 2 ^ core) * 256 + inside
    pieces = list(prep(spot, raw_values))
    copies = jnp.broadcast_to(jnp.pad(bin_edges, ((0, 0), (0, 1)))[None], (16, PIECE, EDGES))
    copies, pieces[0] = lax.optimization_barrier((copies, pieces[0]))
    mine = lax.all_to_all(
        copies, AXES, split_axis=0, concat_axis=0, axis_index_groups=planes(), tiled=True
    )
    mine = mine.reshape(512, EDGES)
    sent = [value.reshape(2, 512, 128) for value in pieces[: 1 + len(EARLY)]]
    halves = [value.reshape(512, 128) for value in pieces[1 + len(EARLY) :]]
    arrived = [sent[0]]
    for (dy, dx), value in zip(EARLY, sent[1:]):
        arrived.append(to_chip(value, dy, dx))
    direct = []
    for i, (dy, dx) in enumerate(LATE):
        for dc in range(2):
            direct.append(to_chip(halves[2 * i + dc], dy, dx, dc))

    wanted = bundle * SPAN + jnp.arange(SPAN, dtype=jnp.int32)
    named = feature_column[None, :] == wanted[:, None]
    feature = jnp.max(jnp.where(named, jnp.arange(FEATURES, dtype=jnp.int32)[None], 0), axis=1)
    offset = jnp.max(jnp.where(named, bin_offset[None], 0), axis=1)
    device = feature // PIECE
    far_y = (device // 64) * 2 + (device // 8) % 2
    line = (far_y * SIDE + (device // 2) % SIDE) * PIECE + feature % PIECE
    line = jnp.where(device % 2 == core, line, line + 512)
    line = jnp.where((device // 16) % SIDE == z, line, 1024)
    part = choose(line, mine, swap_cores(mine))
    turned = []
    for step in (1, 3, 2):
        turned.append(along_z(part, step))
    table = make_table([part] + turned, offset[None])
    parts = []
    for value in arrived:
        parts += [value, swap_cores(value)]
    out = bin_chips(((0, 0), *EARLY), table, parts, None)
    *middle, out = lax.optimization_barrier((*direct[:2], out))
    out = bin_chips(LATE[:1], table, middle, out)
    *last, out = lax.optimization_barrier((*direct[2:], out))
    return bin_chips(LATE[1:], table, last, out)


def solution(mesh):
    in_specs = (P(AXES, None), P(AXES, None), P(), P())
    return jax.shard_map(step, mesh=mesh, in_specs=in_specs, out_specs=P("rows", "bundle"), check_vma=False)
```

```python
import jax
import jax.numpy as jnp
from jax import lax
from jax.experimental import pallas as pl
from jax.experimental.pallas import tpu as pltpu
from jax.sharding import PartitionSpec as P


AXES = ("rows", "bundle")
SIDE = 4
PIECE = 32
EDGES = 256
SPAN = 256
FEATURES = 4096
EARLY = ((1, 0), (0, 2), (1, 1), (0, 3))
LATE = ((1, 3), (0, 1), (1, 2))
GROUP = 1024
SUB = 256


CUTS = [((dy * SIDE + dx) * 512, 512) for dy, dx in ((0, 0), *EARLY)]
CUTS += [((dy * SIDE + dx) * 512 + dc * 256, 256) for dy, dx in LATE for dc in range(2)]


def device_at(y, z, x, core):
    return ((y // 2) * 4 + z) * 16 + (y % 2) * 8 + x * 2 + core


def planes():
    ring = range(SIDE)
    return [[device_at(y, z, x, core) for y in ring for x in ring] for z in ring for core in range(2)]


def along_z(value, step):
    pairs = [(h * SIDE + (z + step) % SIDE, h * SIDE + z) for h in range(2) for z in range(SIDE)]
    return lax.ppermute(value, "rows", pairs)


def swap_cores(value):
    return lax.ppermute(value, "bundle", [(i, i ^ 1) for i in range(16)])


def to_chip(value, dy, dx, dc=0):
    pairs = []
    for y in range(2):
        for x in range(SIDE):
            for core in range(2):
                pairs.append((y * 8 + x * 2 + core, (y ^ dy) * 8 + (x + dx) % SIDE * 2 + (core ^ dc)))
    return lax.ppermute(value, "bundle", pairs)


def pick(table, index):
    dims = lax.GatherDimensionNumbers(
        offset_dims=(),
        collapsed_slice_dims=(0,),
        start_index_map=(0,),
        operand_batching_dims=(1,),
        start_indices_batching_dims=(1,),
    )
    return lax.gather(
        table, index[..., None], dims, (1, 1), mode=lax.GatherScatterMode.PROMISE_IN_BOUNDS
    )


def count_below(values, table):
    top = table(31)
    group = jnp.where(values > jnp.broadcast_to(top[3:4], values.shape), 4, 0)
    group = jnp.where(values > pick(top, group + 1), group + 2, group)
    group = jnp.where(values > pick(top, group), group + 1, group)

    def at(o):
        return pick(table(o), group)

    b4 = values > at(15)
    b5 = values > jnp.where(b4, at(23), at(7))
    b6 = values > jnp.where(b4, jnp.where(b5, at(27), at(19)), jnp.where(b5, at(11), at(3)))

    def among(o):
        pairs = [jnp.where(b6, at(8 * i + 4 + o), at(8 * i + o)) for i in range(4)]
        return jnp.where(b4, jnp.where(b5, pairs[3], pairs[2]), jnp.where(b5, pairs[1], pairs[0]))

    b7 = values > among(1)
    b8 = values > jnp.where(b7, among(2), among(0))
    count = group * 32
    for bit, weight in ((b4, 16), (b5, 8), (b6, 4), (b7, 2), (b8, 1)):
        count = count + jnp.where(bit, weight, 0)
    return count


def prep_kernel(spot_ref, raw_ref, *refs):
    outs = refs[: len(CUTS)]
    buffer, sems, *turned = refs[len(CUTS) :]
    i = pl.program_id(0)

    def turn(j):
        flat = raw_ref[:, j * SUB : (j + 1) * SUB].T
        turned[j][pl.ds(0, SUB, stride=2), :] = flat[:, :128]
        turned[j][pl.ds(1, SUB, stride=2), :] = flat[:, 128:]

    def scatter(j):
        base = i * GROUP + j * SUB
        for start in range(0, SUB, 32):
            rows = []
            for q in range(8):
                four = turned[j][2 * start + 8 * q : 2 * start + 8 * q + 8, :]
                rows += [four[2 * k : 2 * k + 2, :] for k in range(4)]
            for k in range(32):
                buffer[spot_ref[base + start + k]] = rows[k]

    turn(0)
    for j in range(len(turned)):
        if j + 1 < len(turned):
            turn(j + 1)
        scatter(j)

    @pl.when(i == pl.num_programs(0) - 1)
    def _():
        copies = []
        for k, (ref, (start, size)) in enumerate(zip(outs, CUTS)):
            copies.append(pltpu.make_async_copy(buffer.at[pl.ds(start, size)], ref, sems.at[k]))
        for copy in copies:
            copy.start()
        for copy in copies:
            copy.wait()


def prep(spot, raw):
    return pl.pallas_call(
        prep_kernel,
        grid_spec=pltpu.PrefetchScalarGridSpec(
            num_scalar_prefetch=1,
            grid=(FEATURES // GROUP,),
            in_specs=[pl.BlockSpec((256, GROUP), lambda i, c: (0, i))],
            out_specs=[pl.BlockSpec(memory_space=pltpu.HBM)] * len(CUTS),
            scratch_shapes=[pltpu.VMEM((FEATURES, 2, 128), jnp.float32), pltpu.SemaphoreType.DMA((len(CUTS),))]
            + [pltpu.VMEM((SUB * 2, 128), jnp.float32)] * (GROUP // SUB),
        ),
        out_shape=[jax.ShapeDtypeStruct((size, 2, 128), jnp.float32) for _, size in CUTS],
        name="prep",
    )(spot, raw)


def choose_kernel(row_ref, mine_ref, other_ref, out_ref, pool):
    pool[0:512, :] = mine_ref[...]
    pool[512:1024, :] = other_ref[...]
    pool[1024:1032, :] = jnp.zeros((8, EDGES), jnp.float32)

    def eight(i, carry):
        rows = [pool[pl.ds(row_ref[i * 8 + k], 1), :] for k in range(8)]
        out_ref[pl.ds(pl.multiple_of(i * 8, 8), 8), :] = jnp.concatenate(rows, axis=0)
        return carry

    lax.fori_loop(0, SPAN // 8, eight, 0)


def choose(row, mine, other):
    whole = pl.BlockSpec((512, EDGES), lambda i, r: (0, 0))
    return pl.pallas_call(
        choose_kernel,
        grid_spec=pltpu.PrefetchScalarGridSpec(
            num_scalar_prefetch=1,
            grid=(1,),
            in_specs=[whole, whole],
            out_specs=pl.BlockSpec((SPAN, EDGES), lambda i, r: (0, 0)),
            scratch_shapes=[pltpu.VMEM((1032, EDGES), jnp.float32)],
        ),
        out_shape=jax.ShapeDtypeStruct((SPAN, EDGES), jnp.float32),
        name="choose",
    )(row, mine, other)


def table_kernel(a_ref, b_ref, c_ref, d_ref, offset_ref, out_ref, turned):
    total = (a_ref[...] + b_ref[...]) + (c_ref[...] + d_ref[...])
    for half in range(2):
        turned[half] = total[half * 128 : half * 128 + 128, :].T
    for o in range(32):
        for half in range(2):
            lanes = slice(half * 128, half * 128 + 128)
            out_ref[8 * o : 8 * o + 8, lanes] = turned[half, pl.ds(o, 8, stride=32), :]
    out_ref[EDGES - 1 :, :] = offset_ref[...].astype(jnp.float32)


def make_table(parts, offset):
    return pl.pallas_call(
        table_kernel,
        out_shape=jax.ShapeDtypeStruct((EDGES, SPAN), jnp.float32),
        scratch_shapes=[pltpu.VMEM((2, EDGES, 128), jnp.float32)],
        name="make_table",
    )(*parts, offset)


def bin_kernel(table_hbm, *refs, chips, fresh):
    count = len(chips)
    parts = refs[: 2 * count]
    bundle = lax.axis_index("bundle")
    x, y_low, core = (bundle // 2) % SIDE, bundle // 8, bundle % 2
    out_ref, stage, turned, result, table_ref, bases, in_sems, out_sems = refs[2 * count + (0 if fresh else 1) :]

    def take(i, side):
        source = parts[2 * i + side]
        source = source.at[side] if len(source.shape) == 3 else source
        return pltpu.make_async_copy(source, stage.at[2 * i + side], in_sems.at[2 * i + side])

    for i, (dy, dx) in enumerate(chips):
        base = (jnp.where(y_low == dy, 0, SIDE) + (x - dx + SIDE) % SIDE) * 512
        bases[2 * i] = base + core * 256
        bases[2 * i + 1] = base + (1 - core) * 256

    def give(tile):
        part = tile // 4
        rows = pl.ds(pl.multiple_of(bases[part] + (tile % 2) * 128, 128), 128)
        lanes = pl.ds(pl.multiple_of((tile % 4 // 2) * 128, 128), 128)
        return pltpu.make_async_copy(result.at[tile], out_ref.at[rows, lanes], out_sems.at[tile])

    tables = pltpu.make_async_copy(table_hbm, table_ref, in_sems.at[2 * count])
    for i in range(count):
        take(i, 0).start()
        if i == 0:
            tables.start()
        take(i, 1).start()

    def arrive(part):
        pltpu.make_async_copy(stage.at[0], stage.at[part], in_sems.at[part]).wait()

    def turn(tile, slot):
        line = (tile % 4 // 2) * 256 + tile % 2
        turned[slot] = stage[tile // 4, pl.ds(line, 128, stride=2), :].T

    arrive(0)
    turn(0, 0)
    tables.wait()
    last = 8 * count - 1

    def one_tile(t, carry):
        following = jnp.minimum(t + 1, last)

        @pl.when((t % 4 == 3) & (t < last))
        def _():
            arrive(following // 4)

        lanes = pl.ds(pl.multiple_of((t % 4 // 2) * 128, 128), 128)
        offset = jnp.broadcast_to(table_ref[EDGES - 1 :, lanes].astype(jnp.int32), (8, 128))
        for r in range(0, 128, 8):
            below = count_below(
                turned[t % 2, r : r + 8, :], lambda o: table_ref[8 * o : 8 * o + 8, lanes]
            )
            result[t, r : r + 8, :] = below + offset
        turn(following, 1 - t % 2)
        give(t).start()
        return carry

    lax.fori_loop(0, 8 * count, one_tile, 0)

    def drain(t, carry):
        give(t).wait()
        return carry

    lax.fori_loop(0, 8 * count, drain, 0)


def bin_chips(chips, table, parts, out):
    count, fresh = len(chips), out is None
    anywhere = pl.BlockSpec(memory_space=pltpu.HBM)
    return pl.pallas_call(
        lambda *refs: bin_kernel(*refs, chips=chips, fresh=fresh),
        in_specs=[anywhere] * (1 + 2 * count + (0 if fresh else 1)),
        out_specs=anywhere,
        scratch_shapes=[
            pltpu.VMEM((2 * count, 512, 128), jnp.float32),
            pltpu.VMEM((2, 128, 128), jnp.float32),
            pltpu.VMEM((8 * count, 128, 128), jnp.int32),
            pltpu.VMEM((EDGES, SPAN), jnp.float32),
            pltpu.SMEM((2 * count,), jnp.int32),
            pltpu.SemaphoreType.DMA((2 * count + 1,)),
            pltpu.SemaphoreType.DMA((8 * count,)),
        ],
        out_shape=jax.ShapeDtypeStruct((16 * 256, SPAN), jnp.int32),
        input_output_aliases={} if fresh else {1 + 2 * count: 0},
    )(table, *parts, *([] if fresh else [out]))


def step(raw_values, bin_edges, feature_column, bin_offset):
    row, bundle = lax.axis_index("rows"), lax.axis_index("bundle")
    z, core = row % SIDE, bundle % 2
    copies = jnp.broadcast_to(jnp.pad(bin_edges, ((0, 0), (0, 1)))[None], (16, PIECE, EDGES))
    mine = lax.all_to_all(copies, AXES, split_axis=0, concat_axis=0, axis_index_groups=planes(), tiled=True)
    mine = mine.reshape(512, EDGES)

    x, y_low = (bundle // 2) % SIDE, bundle // 8
    owner, inside = feature_column // SPAN, feature_column % SPAN
    chip = (owner // 8 ^ y_low) * SIDE + ((owner // 2) % SIDE - x) % SIDE
    spot = chip * 512 + (owner % 2 ^ core) * 256 + inside
    pieces = list(prep(spot, raw_values))
    sent = [value.reshape(2, 512, 128) for value in pieces[: 1 + len(EARLY)]]
    halves = [value.reshape(512, 128) for value in pieces[1 + len(EARLY) :]]
    arrived = [sent[0]]
    for (dy, dx), value in zip(EARLY, sent[1:]):
        arrived.append(to_chip(value, dy, dx))
    direct = []
    for i, (dy, dx) in enumerate(LATE):
        for dc in range(2):
            direct.append(to_chip(halves[2 * i + dc], dy, dx, dc))

    wanted = bundle * SPAN + jnp.arange(SPAN, dtype=jnp.int32)
    named = feature_column[None, :] == wanted[:, None]
    feature = jnp.max(jnp.where(named, jnp.arange(FEATURES, dtype=jnp.int32)[None], 0), axis=1)
    offset = jnp.max(jnp.where(named, bin_offset[None], 0), axis=1)
    device = feature // PIECE
    far_y = (device // 64) * 2 + (device // 8) % 2
    line = (far_y * SIDE + (device // 2) % SIDE) * PIECE + feature % PIECE
    line = jnp.where(device % 2 == core, line, line + 512)
    line = jnp.where((device // 16) % SIDE == z, line, 1024)
    part = choose(line, mine, swap_cores(mine))
    turned = []
    for step in (1, 3, 2):
        turned.append(along_z(part, step))
    table = make_table([part] + turned, offset[None])
    parts = []
    for value in arrived:
        parts += [value, swap_cores(value)]
    out = bin_chips(((0, 0), *EARLY), table, parts, None)
    *middle, out = lax.optimization_barrier((*direct[2:4], out))
    out = bin_chips(LATE[1:2], table, middle, out)
    last = direct[0:2] + direct[4:6]
    *last, out = lax.optimization_barrier((*last, out))
    return bin_chips((LATE[0], LATE[2]), table, last, out)


def solution(mesh):
    in_specs = (P(AXES, None), P(AXES, None), P(), P())
    return jax.shard_map(step, mesh=mesh, in_specs=in_specs, out_specs=P("rows", "bundle"), check_vma=False)
```

```python
import jax
import jax.numpy as jnp
from jax import lax
from jax.experimental import pallas as pl
from jax.experimental.pallas import tpu as pltpu
from jax.sharding import PartitionSpec as P


AXES = ("rows", "bundle")
SIDE = 4
PIECE = 32
EDGES = 256
SPAN = 256
FEATURES = 4096
EARLY = ((1, 0), (0, 2), (1, 1), (0, 3))
LATE = ((1, 3), (0, 1), (1, 2))
GROUP = 1024
SUB = 256


CUTS = [((dy * SIDE + dx) * 512, 512) for dy, dx in ((0, 0), *EARLY)]
CUTS += [((dy * SIDE + dx) * 512 + dc * 256, 256) for dy, dx in LATE for dc in range(2)]


def device_at(y, z, x, core):
    return ((y // 2) * 4 + z) * 16 + (y % 2) * 8 + x * 2 + core


def planes():
    ring = range(SIDE)
    return [[device_at(y, z, x, core) for y in ring for x in ring] for z in ring for core in range(2)]


def along_z(value, step):
    pairs = [(h * SIDE + (z + step) % SIDE, h * SIDE + z) for h in range(2) for z in range(SIDE)]
    return lax.ppermute(value, "rows", pairs)


def swap_cores(value):
    return lax.ppermute(value, "bundle", [(i, i ^ 1) for i in range(16)])


def to_chip(value, dy, dx, dc=0):
    pairs = []
    for y in range(2):
        for x in range(SIDE):
            for core in range(2):
                pairs.append((y * 8 + x * 2 + core, (y ^ dy) * 8 + (x + dx) % SIDE * 2 + (core ^ dc)))
    return lax.ppermute(value, "bundle", pairs)


def pick(table, index):
    dims = lax.GatherDimensionNumbers(
        offset_dims=(),
        collapsed_slice_dims=(0,),
        start_index_map=(0,),
        operand_batching_dims=(1,),
        start_indices_batching_dims=(1,),
    )
    return lax.gather(
        table, index[..., None], dims, (1, 1), mode=lax.GatherScatterMode.PROMISE_IN_BOUNDS
    )


def count_below(values, table):
    top = table(31)
    group = jnp.where(values > jnp.broadcast_to(top[3:4], values.shape), 4, 0)
    group = jnp.where(values > pick(top, group + 1), group + 2, group)
    group = jnp.where(values > pick(top, group), group + 1, group)

    def at(o):
        return pick(table(o), group)

    b4 = values > at(15)
    b5 = values > jnp.where(b4, at(23), at(7))
    b6 = values > jnp.where(b4, jnp.where(b5, at(27), at(19)), jnp.where(b5, at(11), at(3)))

    def among(o):
        pairs = [jnp.where(b6, at(8 * i + 4 + o), at(8 * i + o)) for i in range(4)]
        return jnp.where(b4, jnp.where(b5, pairs[3], pairs[2]), jnp.where(b5, pairs[1], pairs[0]))

    b7 = values > among(1)
    b8 = values > jnp.where(b7, among(2), among(0))
    count = group * 32
    for bit, weight in ((b4, 16), (b5, 8), (b6, 4), (b7, 2), (b8, 1)):
        count = count + jnp.where(bit, weight, 0)
    return count


def prep_kernel(column_ref, raw_ref, *refs):
    outs = refs[: len(CUTS)]
    buffer, sems, vector_spots, spots, *turned = refs[len(CUTS) :]
    i = pl.program_id(0)

    def turn(j):
        flat = raw_ref[:, j * SUB : (j + 1) * SUB].T
        turned[j][pl.ds(0, SUB, stride=2), :] = flat[:, :128]
        turned[j][pl.ds(1, SUB, stride=2), :] = flat[:, 128:]

    def scatter(j):
        base = i * (GROUP // 128) + j * (SUB // 128)
        for start in range(0, SUB, 32):
            rows = []
            for q in range(8):
                four = turned[j][2 * start + 8 * q : 2 * start + 8 * q + 8, :]
                rows += [four[2 * k : 2 * k + 2, :] for k in range(4)]
            for k in range(32):
                buffer[spots[base + (start + k) // 128, (start + k) % 128]] = rows[k]

    load = pltpu.make_async_copy(vector_spots, spots, sems.at[len(CUTS)])

    @pl.when(i == 0)
    def _():
        bundle, column = lax.axis_index("bundle"), column_ref[...]
        far_x = ((column >> 9) - ((bundle >> 1) & 3)) & 3
        chip = (((column >> 11) ^ (bundle >> 3)) << 2) | far_x
        far_core = ((column >> 8) ^ bundle) & 1
        vector_spots[...] = (chip << 9) | (far_core << 8) | (column & 255)
        load.start()

    turn(0)

    @pl.when(i == 0)
    def _():
        load.wait()

    for j in range(len(turned)):
        if j + 1 < len(turned):
            turn(j + 1)
        scatter(j)

    @pl.when(i == pl.num_programs(0) - 1)
    def _():
        copies = []
        for k, (ref, (start, size)) in enumerate(zip(outs, CUTS)):
            copies.append(pltpu.make_async_copy(buffer.at[pl.ds(start, size)], ref, sems.at[k]))
        for copy in copies:
            copy.start()
        for copy in copies:
            copy.wait()


def prep(column, raw):
    return pl.pallas_call(
        prep_kernel,
        grid_spec=pltpu.PrefetchScalarGridSpec(
            num_scalar_prefetch=0,
            grid=(FEATURES // GROUP,),
            in_specs=[
                pl.BlockSpec((FEATURES // 128, 128), lambda i: (0, 0)),
                pl.BlockSpec((256, GROUP), lambda i: (0, i)),
            ],
            out_specs=[pl.BlockSpec(memory_space=pltpu.HBM)] * len(CUTS),
            scratch_shapes=[pltpu.VMEM((FEATURES, 2, 128), jnp.float32), pltpu.SemaphoreType.DMA((len(CUTS) + 1,))]
            + [pltpu.VMEM((FEATURES // 128, 128), jnp.int32), pltpu.SMEM((FEATURES // 128, 128), jnp.int32)]
            + [pltpu.VMEM((SUB * 2, 128), jnp.float32)] * (GROUP // SUB),
        ),
        out_shape=[jax.ShapeDtypeStruct((size, 2, 128), jnp.float32) for _, size in CUTS],
        name="prep",
    )(column.reshape(FEATURES // 128, 128), raw)


def choose_kernel(row_ref, mine_ref, other_ref, out_ref, pool):
    pool[0:512, :] = mine_ref[...]
    pool[512:1024, :] = other_ref[...]
    pool[1024:1032, :] = jnp.zeros((8, EDGES), jnp.float32)

    def eight(i, carry):
        rows = [pool[pl.ds(row_ref[i * 8 + k], 1), :] for k in range(8)]
        out_ref[pl.ds(pl.multiple_of(i * 8, 8), 8), :] = jnp.concatenate(rows, axis=0)
        return carry

    lax.fori_loop(0, SPAN // 8, eight, 0)


def choose(row, mine, other):
    whole = pl.BlockSpec((512, EDGES), lambda i, r: (0, 0))
    return pl.pallas_call(
        choose_kernel,
        grid_spec=pltpu.PrefetchScalarGridSpec(
            num_scalar_prefetch=1,
            grid=(1,),
            in_specs=[whole, whole],
            out_specs=pl.BlockSpec((SPAN, EDGES), lambda i, r: (0, 0)),
            scratch_shapes=[pltpu.VMEM((1032, EDGES), jnp.float32)],
        ),
        out_shape=jax.ShapeDtypeStruct((SPAN, EDGES), jnp.float32),
        name="choose",
    )(row, mine, other)


def table_kernel(a_ref, b_ref, c_ref, d_ref, offset_ref, out_ref, turned):
    total = (a_ref[...] + b_ref[...]) + (c_ref[...] + d_ref[...])
    for half in range(2):
        turned[half] = total[half * 128 : half * 128 + 128, :].T
    for o in range(32):
        for half in range(2):
            lanes = slice(half * 128, half * 128 + 128)
            out_ref[8 * o : 8 * o + 8, lanes] = turned[half, pl.ds(o, 8, stride=32), :]
    out_ref[EDGES - 1 :, :] = offset_ref[...].astype(jnp.float32)


def make_table(parts, offset):
    return pl.pallas_call(
        table_kernel,
        out_shape=jax.ShapeDtypeStruct((EDGES, SPAN), jnp.float32),
        scratch_shapes=[pltpu.VMEM((2, EDGES, 128), jnp.float32)],
        name="make_table",
    )(*parts, offset)


def bin_kernel(table_hbm, *refs, chips, fresh):
    count = len(chips)
    parts = refs[: 2 * count]
    bundle = lax.axis_index("bundle")
    x, y_low, core = (bundle // 2) % SIDE, bundle // 8, bundle % 2
    out_ref, stage, turned, result, table_ref, bases, in_sems, out_sems = refs[2 * count + (0 if fresh else 1) :]

    def take(i, side):
        source = parts[2 * i + side]
        source = source.at[side] if len(source.shape) == 3 else source
        return pltpu.make_async_copy(source, stage.at[2 * i + side], in_sems.at[2 * i + side])

    for i, (dy, dx) in enumerate(chips):
        base = (jnp.where(y_low == dy, 0, SIDE) + (x - dx + SIDE) % SIDE) * 512
        bases[2 * i] = base + core * 256
        bases[2 * i + 1] = base + (1 - core) * 256

    def give(tile):
        part = tile // 4
        rows = pl.ds(pl.multiple_of(bases[part] + (tile % 2) * 128, 128), 128)
        lanes = pl.ds(pl.multiple_of((tile % 4 // 2) * 128, 128), 128)
        return pltpu.make_async_copy(result.at[tile], out_ref.at[rows, lanes], out_sems.at[tile])

    tables = pltpu.make_async_copy(table_hbm, table_ref, in_sems.at[2 * count])
    for i in range(count):
        take(i, 0).start()
        if i == 0:
            tables.start()
        take(i, 1).start()

    def arrive(part):
        pltpu.make_async_copy(stage.at[0], stage.at[part], in_sems.at[part]).wait()

    def turn(tile, slot):
        line = (tile % 4 // 2) * 256 + tile % 2
        turned[slot] = stage[tile // 4, pl.ds(line, 128, stride=2), :].T

    arrive(0)
    turn(0, 0)
    tables.wait()
    last = 8 * count - 1

    def one_tile(t, carry):
        following = jnp.minimum(t + 1, last)

        @pl.when((t % 4 == 3) & (t < last))
        def _():
            arrive(following // 4)

        lanes = pl.ds(pl.multiple_of((t % 4 // 2) * 128, 128), 128)
        offset = jnp.broadcast_to(table_ref[EDGES - 1 :, lanes].astype(jnp.int32), (8, 128))
        for r in range(0, 128, 8):
            below = count_below(
                turned[t % 2, r : r + 8, :], lambda o: table_ref[8 * o : 8 * o + 8, lanes]
            )
            result[t, r : r + 8, :] = below + offset
        turn(following, 1 - t % 2)
        give(t).start()
        return carry

    lax.fori_loop(0, 8 * count, one_tile, 0)

    def drain(t, carry):
        give(t).wait()
        return carry

    lax.fori_loop(0, 8 * count, drain, 0)


def bin_chips(chips, table, parts, out):
    count, fresh = len(chips), out is None
    anywhere = pl.BlockSpec(memory_space=pltpu.HBM)
    return pl.pallas_call(
        lambda *refs: bin_kernel(*refs, chips=chips, fresh=fresh),
        in_specs=[anywhere] * (1 + 2 * count + (0 if fresh else 1)),
        out_specs=anywhere,
        scratch_shapes=[
            pltpu.VMEM((2 * count, 512, 128), jnp.float32),
            pltpu.VMEM((2, 128, 128), jnp.float32),
            pltpu.VMEM((8 * count, 128, 128), jnp.int32),
            pltpu.VMEM((EDGES, SPAN), jnp.float32),
            pltpu.SMEM((2 * count,), jnp.int32),
            pltpu.SemaphoreType.DMA((2 * count + 1,)),
            pltpu.SemaphoreType.DMA((8 * count,)),
        ],
        out_shape=jax.ShapeDtypeStruct((16 * 256, SPAN), jnp.int32),
        input_output_aliases={} if fresh else {1 + 2 * count: 0},
    )(table, *parts, *([] if fresh else [out]))


def step(raw_values, bin_edges, feature_column, bin_offset):
    row, bundle = lax.axis_index("rows"), lax.axis_index("bundle")
    z, core = row % SIDE, bundle % 2
    copies = jnp.broadcast_to(jnp.pad(bin_edges, ((0, 0), (0, 1)))[None], (16, PIECE, EDGES))
    mine = lax.all_to_all(copies, AXES, split_axis=0, concat_axis=0, axis_index_groups=planes(), tiled=True)
    mine = mine.reshape(512, EDGES)

    pieces = list(prep(feature_column, raw_values))
    sent = [value.reshape(2, 512, 128) for value in pieces[: 1 + len(EARLY)]]
    halves = [value.reshape(512, 128) for value in pieces[1 + len(EARLY) :]]
    arrived = [sent[0]]
    for (dy, dx), value in zip(EARLY, sent[1:]):
        arrived.append(to_chip(value, dy, dx))
    direct = []
    for i, (dy, dx) in enumerate(LATE):
        for dc in range(2):
            direct.append(to_chip(halves[2 * i + dc], dy, dx, dc))

    wanted = bundle * SPAN + jnp.arange(SPAN, dtype=jnp.int32)
    named = feature_column[None, :] == wanted[:, None]
    feature = jnp.max(jnp.where(named, jnp.arange(FEATURES, dtype=jnp.int32)[None], 0), axis=1)
    offset = jnp.max(jnp.where(named, bin_offset[None], 0), axis=1)
    device = feature // PIECE
    far_y = (device // 64) * 2 + (device // 8) % 2
    line = (far_y * SIDE + (device // 2) % SIDE) * PIECE + feature % PIECE
    line = jnp.where(device % 2 == core, line, line + 512)
    line = jnp.where((device // 16) % SIDE == z, line, 1024)
    part = choose(line, mine, swap_cores(mine))
    turned = []
    for step in (1, 3, 2):
        turned.append(along_z(part, step))
    table = make_table([part] + turned, offset[None])
    parts = []
    for value in arrived:
        parts += [value, swap_cores(value)]
    out = bin_chips(((0, 0), *EARLY), table, parts, None)
    *middle, out = lax.optimization_barrier((*direct[2:4], out))
    out = bin_chips(LATE[1:2], table, middle, out)
    last = direct[0:2] + direct[4:6]
    *last, out = lax.optimization_barrier((*last, out))
    return bin_chips((LATE[0], LATE[2]), table, last, out)


def solution(mesh):
    in_specs = (P(AXES, None), P(AXES, None), P(), P())
    return jax.shard_map(step, mesh=mesh, in_specs=in_specs, out_specs=P("rows", "bundle"), check_vma=False)
```
